32 devices in a mesh: section: 4 (over y, x), dp: 8 (over z, core).
Axes of the slice: x: 2, y: 2, z: 4, core: 2. Of those that a mesh axis runs over, the one named last changes fastest.
Arguments:
- saved_inputs: bfloat16 [4, 2, 1024, 320], P('section', None, 'dp'), may hold values from -6 to 6
- timesteps: int32 [2, 1024], P(None, 'dp'), may hold values from 0 to 999
- time_table: bfloat16 [1000, 320], replicated, may hold values from -6 to 6
- skip_weight: bfloat16 [4, 320, 320], P('section'), may hold values from -0.3125 to 0.3125
- ff_in: bfloat16 [4, 1280, 320], P('section'), may hold values from -0.3125 to 0.3125
- ff_out: bfloat16 [4, 1280, 320], P('section'), may hold values from -0.15625 to 0.15625
- output_cotangent: bfloat16 [2, 1024, 320], P(None, 'dp'), may hold values from -6 to 6
Outputs:
- input_grads: bfloat16 [4, 2, 1024, 320], P('section', None, 'dp')
- skip_weight_grad: float32 [4, 102400], P('section', 'dp')
- ff_in_grad: float32 [4, 1280, 320], P('section', 'dp')
- ff_out_grad: float32 [4, 1280, 320], P('section', 'dp')
The draws below stay inside these ranges and needn't reach their ends.
All inputs are finite; a program needn't handle non-finite values.
Results may differ from the reference program's by a relative error of at most 0.01.
Values may be sent and summed in bfloat16 or wider, within the bound.
A program may use at most 128 MiB of HBM per device.

```python
import jax
import jax.numpy as jnp
from jax import lax

C = 320
F = 1280
NT = 1000
M = 2
ROWS = 1024
N_SECTION = 4


def touch_ends(values, own_key, low, largest):
    longest = values.shape.index(max(values.shape))
    spots = []
    for shift in (0, 1):
        where = [jax.random.randint(jax.random.fold_in(own_key, axis), (), 0, length) for axis, length in enumerate(values.shape)]
        where[longest] = (where[longest] + shift) % values.shape[longest]
        spots.append(tuple(where))
    return values.at[spots[0]].set(low).at[spots[1]].set(largest)


def block_levels(stream_key, shape, cuts, least, top_value):
    def one(axis_at, blocks):
        draws = jax.random.uniform(jax.random.fold_in(jax.random.fold_in(stream_key, 6), axis_at), (blocks,), jnp.float32, least / len(cuts), top_value / len(cuts))
        return jnp.repeat(jnp.exp(draws), shape[axis_at] // blocks).reshape((-1,) + (1,) * (len(shape) - axis_at - 1))

    gain = one(*cuts[0])
    for cut in cuts[1:]:
        gain = gain * one(*cut)
    return gain


def normal_values(stream_key, extent, spread, reach, shards=(), kind=jnp.bfloat16):
    array = spread * jax.random.normal(stream_key, extent, jnp.float32)
    if shards:
        array = array * block_levels(stream_key, extent, shards, -0.22, 0.18)
    return jnp.clip(array, -reach, reach).astype(kind)


def setup_inputs(seed: int = 0) -> dict:
    key_list = jax.random.split(jax.random.key(seed), 8)
    return {
        "saved_inputs": normal_values(key_list[0], (N_SECTION, M, ROWS, C), 1.0, 6.0, ((0, 4), (2, 8))),
        "timesteps": touch_ends(jax.random.randint(key_list[1], (M, ROWS), 0, NT), jax.random.fold_in(key_list[1], 1), 0, NT - 1).astype(jnp.int32),
        "time_table": normal_values(key_list[2], (NT, C), 1.0, 6.0),
        "skip_weight": normal_values(key_list[3], (N_SECTION, C, C), C ** -0.5, 0.3125, ((0, 4),)),
        "ff_in": normal_values(key_list[4], (N_SECTION, F, C), C ** -0.5, 0.3125, ((0, 4),)),
        "ff_out": normal_values(key_list[5], (N_SECTION, F, C), F ** -0.5, 0.15625, ((0, 4),)),
        "output_cotangent": normal_values(key_list[6], (M, ROWS, C), 1.0, 6.0, ((1, 8),)),
    }


EPS = 1e-06

def contract(left, right, dims):
    return lax.dot_general(left, right, ((dims[0], dims[1]), ((), ())), preferred_element_type=jnp.float32)

def forward(inputs, source, w_skip, w_in, w_out):
    united = inputs.astype(jnp.float32) + jnp.dot(source, w_skip, preferred_element_type=jnp.float32)
    recip = lax.rsqrt(lax.optimization_barrier(jnp.mean(united * united, axis=-1, keepdims=True)) + EPS)
    normed = (united * recip).astype(jnp.bfloat16)
    preact = contract(normed, w_in, ((1,), (1,)))
    active = jax.nn.silu(preact).astype(jnp.bfloat16)
    output = united + jnp.dot(active, w_out, preferred_element_type=jnp.float32)
    return (united, recip, normed, preact, active, output)

def backward(grad_out, inputs, source, w_skip, w_in, w_out):
    united, recip, normed, preact, active, output = forward(inputs, source, w_skip, w_in, w_out)
    grad_low = grad_out.astype(jnp.bfloat16)
    grad_act = contract(grad_low, w_out, ((1,), (1,)))
    sigma = jax.nn.sigmoid(preact)
    grad_pre = (grad_act * sigma * (1.0 + preact * (1.0 - sigma))).astype(jnp.bfloat16)
    d_in = contract(grad_pre, normed, ((0,), (0,)))
    d_out = contract(active, grad_low, ((0,), (0,)))
    grad_norm = jnp.dot(grad_pre, w_in, preferred_element_type=jnp.float32)
    grad_united = grad_out + recip * grad_norm - united * recip ** 3 * lax.optimization_barrier(jnp.mean(grad_norm * united, axis=-1, keepdims=True))
    united_low = grad_united.astype(jnp.bfloat16)
    d_skip = contract(source, united_low, ((0,), (0,)))
    grad_source = contract(united_low, w_skip, ((1,), (1,))).astype(jnp.bfloat16)
    return (united_low, grad_source, d_in, d_out, d_skip)

def reference(saved_inputs, timesteps, time_table, skip_weight, ff_in, ff_out, output_cotangent):
    grads = [[None] * M for section in range(4)]
    sum_in = [jnp.zeros((F, C), jnp.float32) for section in range(4)]
    sum_out = [jnp.zeros((F, C), jnp.float32) for section in range(4)]
    sum_skip = [jnp.zeros((C, C), jnp.float32) for section in range(4)]
    for micro in range(M):
        embeds = jnp.take(time_table, timesteps[micro], axis=0)
        values = []
        for section in range(2):
            output = forward(saved_inputs[section, micro], embeds, skip_weight[section], ff_in[section], ff_out[section])[5]
            values.append(output.astype(jnp.bfloat16))
        pending = [None, None]
        chain = None
        for section in (3, 2, 1, 0):
            if section == 3:
                grad_out = output_cotangent[micro].astype(jnp.float32)
            elif section == 2:
                grad_out = chain.astype(jnp.float32)
            else:
                grad_out = chain.astype(jnp.float32) + pending[section].astype(jnp.float32)
            source = values[3 - section] if section >= 2 else embeds
            parts = backward(grad_out, saved_inputs[section, micro], source, skip_weight[section], ff_in[section], ff_out[section])
            chain = parts[0]
            if section >= 2:
                pending[3 - section] = parts[1]
            grads[section][micro] = chain
            sum_in[section] = sum_in[section] + parts[2]
            sum_out[section] = sum_out[section] + parts[3]
            sum_skip[section] = sum_skip[section] + parts[4]
    input_grads = jnp.stack([jnp.stack(grads[section]) for section in range(4)])
    skip_grad = jnp.stack([sum_skip[section].reshape(-1) for section in range(4)])
    return (input_grads, skip_grad, jnp.stack(sum_in), jnp.stack(sum_out))
```

```python
import functools

import jax
import jax.numpy as jnp
from jax import lax
from jax.experimental import pallas as pl
from jax.experimental.pallas import tpu as pltpu
from jax.sharding import PartitionSpec as P

EPS = 1e-06
MESH = pl.DeviceIdType.MESH
F32 = jnp.float32
BF16 = jnp.bfloat16


def contract(left, right, dims):
    return lax.dot_general(
        left, right, ((dims[0], dims[1]), ((), ())), preferred_element_type=jnp.float32
    )


def kernel(n_section, n_dp, scatter, *refs):
    (x, ts, table, w_skip, w_in, w_out, cot) = refs[:7]
    (ig, g_skip, g_in, g_out) = refs[7:11]
    (zbuf, ybuf, ubuf, rbuf, nbuf, abuf, dbuf, gbuf, lowbuf, gpbuf, cbuf, kbuf, skbuf) = refs[11:24]
    (vs, vr, cs, cr, ks, kr) = refs[24:30]
    rs = refs[30:]
    sec = lax.axis_index("section")
    dp = lax.axis_index("dp")
    n_micro, rows, width = cot.shape
    hidden = w_in.shape[1]
    half = n_section // 2
    pairs = n_dp // 2
    core = lax.rem(dp, 2)
    place = lax.div(dp, 2)
    mate = dp + 1 - 2 * core

    def remote(src, dst, send, recv, **where):
        return pltpu.make_async_remote_copy(
            src_ref=src, dst_ref=dst, send_sem=send, recv_sem=recv, device_id=where, device_id_type=MESH
        )

    barrier = pltpu.get_barrier_semaphore()
    count = 0
    for k in range(1, n_section):
        pl.semaphore_signal(
            barrier, inc=1, device_id={"section": lax.rem(sec + k, n_section)}, device_id_type=MESH
        )
        count += 1
    if scatter:
        pl.semaphore_signal(barrier, inc=1, device_id={"dp": mate}, device_id_type=MESH)
        count += 1
        for k in range(1, pairs):
            other = lax.rem(place + k, pairs) * 2 + core
            pl.semaphore_signal(barrier, inc=1, device_id={"dp": other}, device_id_type=MESH)
            count += 1

    mirror = n_section - 1 - sec
    below = lax.max(sec - 1, 0)
    values = [remote(ybuf.at[m], zbuf.at[m], vs.at[m], vr.at[m], section=mirror) for m in range(n_micro)]
    chains = [remote(cbuf.at[m], gbuf.at[m], cs.at[m], cr.at[m], section=below) for m in range(n_micro)]
    skips = [remote(kbuf.at[m], skbuf.at[m], ks.at[m], kr.at[m], section=mirror) for m in range(n_micro)]

    def forward(m):
        span = pl.ds(m * rows, rows)
        united = x[0, m].astype(F32) + jnp.dot(zbuf[m], w_skip[0], preferred_element_type=F32)
        recip = lax.rsqrt(jnp.mean(united * united, axis=-1, keepdims=True) + EPS)
        normed = (united * recip).astype(BF16)
        preact = contract(normed, w_in[0], ((1,), (1,)))
        sigma = jax.nn.sigmoid(preact)
        active = (preact * sigma).astype(BF16)
        ubuf[m] = united
        rbuf[m] = recip
        nbuf[span, :] = normed
        abuf[span, :] = active
        dbuf[m] = sigma * (1.0 + preact * (1.0 - sigma))
        return united, active

    @pl.when(sec < half)
    def _():
        levels = lax.broadcasted_iota(jnp.int32, (table.shape[0], rows), 0)
        for m in range(n_micro):
            onehot = (levels == ts[m : m + 1, :]).astype(F32).astype(BF16)
            zbuf[m] = contract(onehot, table[...], ((0,), (0,))).astype(BF16)
            united, active = forward(m)
            output = united + jnp.dot(active, w_out[0], preferred_element_type=F32)
            ybuf[m] = output.astype(BF16)
            if m == 0:
                pl.semaphore_wait(barrier, count)
            values[m].start()

    @pl.when(sec >= half - 1)
    def _():
        skbuf[...] = jnp.zeros_like(skbuf)

    @pl.when(sec >= half)
    def _():
        pl.semaphore_wait(barrier, count)

    for m in range(n_micro):

        @pl.when(sec >= half)
        def _():
            values[m].wait_recv()
            forward(m)

        @pl.when(sec == n_section - 1)
        def _():
            gbuf[m] = cot[m]

        @pl.when(sec < n_section - 1)
        def _():
            chains[m].wait_recv()

        @pl.when(sec < half - 1)
        def _():
            skips[m].wait_recv()

        span = pl.ds(m * rows, rows)
        grad_out = gbuf[m].astype(F32) + skbuf[m].astype(F32)
        grad_low = grad_out.astype(BF16)
        lowbuf[span, :] = grad_low
        grad_act = contract(grad_low, w_out[0], ((1,), (1,)))
        grad_pre = (grad_act * dbuf[m]).astype(BF16)
        gpbuf[span, :] = grad_pre
        grad_norm = jnp.dot(grad_pre, w_in[0], preferred_element_type=F32)
        united = ubuf[m]
        recip = rbuf[m]
        grad_united = (
            grad_out
            + recip * grad_norm
            - united * recip**3 * jnp.mean(grad_norm * united, axis=-1, keepdims=True)
        )
        low = grad_united.astype(BF16)
        ig[0, m] = low

        @pl.when(sec != half)
        def _():
            cbuf[m] = low

            @pl.when(sec > 0)
            def _():
                chains[m].start()

        @pl.when(sec >= half)
        def _():
            back = contract(low, w_skip[0], ((1,), (1,))).astype(BF16)

            @pl.when(sec == half)
            def _():
                cbuf[m] = (low.astype(F32) + back.astype(F32)).astype(BF16)
                chains[m].start()

            @pl.when(sec > half)
            def _():
                kbuf[m] = back
                skips[m].start()

    d_out = contract(abuf[...], lowbuf[...], ((0,), (0,)))
    d_in = contract(gpbuf[...], nbuf[...], ((0,), (0,)))
    d_skip = contract(
        zbuf[...].reshape(n_micro * rows, width), ig[0].reshape(n_micro * rows, width), ((0,), (0,))
    )

    if scatter:
        (acc, pbuf, precv, sbuf, rrecv, ps, pr, ss, sr) = rs
        fh = hidden // n_dp
        kh = width // n_dp
        acc[:, 0:fh, :] = d_in.reshape(n_dp, fh, width)
        acc[:, fh : 2 * fh, :] = d_out.reshape(n_dp, fh, width)
        acc[:, 2 * fh : 2 * fh + kh, :] = d_skip.reshape(n_dp, kh, width)
        first = []
        for t in range(pairs):
            pbuf[t] = acc[2 * t + 1 - core].astype(BF16)
            copy = remote(pbuf.at[t], precv.at[t], ps.at[t], pr.at[t], dp=mate)
            copy.start()
            first.append(copy)
        for copy in first:
            copy.wait_recv()
        second = []
        for k in range(1, pairs):
            t = lax.rem(place + k, pairs)
            sbuf[k] = (acc[2 * t + core] + precv[t].astype(F32)).astype(BF16)
            copy = remote(sbuf.at[k], rrecv.at[k], ss.at[k], sr.at[k], dp=2 * t + core)
            copy.start()
            second.append(copy)
        total = acc[dp] + precv[place].astype(F32)
        for k in range(1, pairs):
            second[k - 1].wait_recv()
            total = total + rrecv[k].astype(F32)
        g_in[...] = total[0:fh]
        g_out[...] = total[fh : 2 * fh]
        g_skip[...] = total[2 * fh : 2 * fh + kh]
        for copy in first + second:
            copy.wait_send()
    else:
        g_in[...] = d_in
        g_out[...] = d_out
        g_skip[...] = d_skip

    for m in range(n_micro):

        @pl.when(sec < half)
        def _():
            values[m].wait_send()

        @pl.when(sec > 0)
        def _():
            chains[m].wait_send()

        @pl.when(sec > half)
        def _():
            skips[m].wait_send()


def shards(n_section, n_dp, saved_inputs, timesteps, time_table, skip_weight, ff_in, ff_out, output_cotangent):
    n_micro, rows, width = output_cotangent.shape
    hidden = ff_in.shape[1]
    pairs = n_dp // 2
    scatter = n_dp % 2 == 0 and hidden % (16 * n_dp) == 0 and width % (8 * n_dp) == 0
    fh = hidden // n_dp if scatter else hidden
    kh = width // n_dp if scatter else width
    stack = 2 * fh + kh
    every = n_micro * rows
    low = pltpu.VMEM((n_micro, rows, width), BF16)
    scratch = [
        low,
        low,
        pltpu.VMEM((n_micro, rows, width), F32),
        pltpu.VMEM((n_micro, rows, 1), F32),
        pltpu.VMEM((every, width), BF16),
        pltpu.VMEM((every, hidden), BF16),
        pltpu.VMEM((n_micro, rows, hidden), F32),
        low,
        pltpu.VMEM((every, width), BF16),
        pltpu.VMEM((every, hidden), BF16),
        low,
        low,
        low,
    ] + [pltpu.SemaphoreType.DMA((n_micro,))] * 6
    if scatter:
        block = pltpu.VMEM((pairs, stack, width), BF16)
        scratch += [pltpu.VMEM((n_dp, stack, width), F32), block, block, block, block]
        scratch += [pltpu.SemaphoreType.DMA((pairs,))] * 4
    grad_store, grad_skip, grad_in, grad_out = pl.pallas_call(
        functools.partial(kernel, n_section, n_dp, scatter),
        out_shape=(
            jax.ShapeDtypeStruct(saved_inputs.shape, BF16),
            jax.ShapeDtypeStruct((kh, width), F32),
            jax.ShapeDtypeStruct((fh, width), F32),
            jax.ShapeDtypeStruct((fh, width), F32),
        ),
        in_specs=[pl.BlockSpec(memory_space=pltpu.VMEM)] * 7,
        out_specs=[pl.BlockSpec(memory_space=pltpu.VMEM)] * 4,
        scratch_shapes=scratch,
        compiler_params=pltpu.CompilerParams(
            collective_id=0, has_side_effects=True, vmem_limit_bytes=60 * 1024 * 1024
        ),
    )(saved_inputs, timesteps, time_table, skip_weight, ff_in, ff_out, output_cotangent)
    grad_skip = grad_skip.reshape(-1)
    if not scatter:
        grad_in, grad_out, grad_skip = (
            lax.psum_scatter(value, "dp", scatter_dimension=0, tiled=True)
            for value in (grad_in, grad_out, grad_skip)
        )
    return (grad_store, grad_skip[None], grad_in[None], grad_out[None])


def solution(mesh):
    in_specs = (
        P("section", None, "dp", None),
        P(None, "dp"),
        P(),
        P("section", None, None),
        P("section", None, None),
        P("section", None, None),
        P(None, "dp", None),
    )
    out_specs = (
        P("section", None, "dp", None),
        P("section", "dp"),
        P("section", "dp", None),
        P("section", "dp", None),
    )
    body = functools.partial(shards, mesh.shape["section"], mesh.shape["dp"])
    return jax.shard_map(body, mesh=mesh, in_specs=in_specs, out_specs=out_specs, check_vma=False)
```

```python
import functools

import jax
import jax.numpy as jnp
from jax import lax
from jax.experimental import pallas as pl
from jax.experimental.pallas import tpu as pltpu
from jax.sharding import PartitionSpec as P

EPS = 1e-06
MESH = pl.DeviceIdType.MESH
F32 = jnp.float32
BF16 = jnp.bfloat16
LANES = 128
CHUNKS = 2


def contract(left, right, dims):
    return lax.dot_general(
        left, right, ((dims[0], dims[1]), ((), ())), preferred_element_type=jnp.float32
    )


def kernel(n_section, n_dp, scatter, *refs):
    (x, ts, table, w_skip, w_in, w_out, cot) = refs[:7]
    (ig, g_skip, g_in, g_out) = refs[7:11]
    (wsk_t, win_n, wout_n, zbuf, zall, ybuf, ubuf, rbuf, nbuf, abuf, dbuf) = refs[11:22]
    (gbuf, lowbuf, gpbuf, gall, cbuf, kbuf, skbuf) = refs[22:29]
    (vs, vr, cs, cr, ks, kr) = refs[29:35]
    rs = refs[35:]
    sec = lax.axis_index("section")
    dp = lax.axis_index("dp")
    n_micro, width, rows = cot.shape
    hidden = w_in.shape[2]
    half = n_section // 2
    pairs = n_dp // 2
    core = lax.rem(dp, 2)
    place = lax.div(dp, 2)
    mate = dp + 1 - 2 * core

    def remote(src, dst, send, recv, **where):
        return pltpu.make_async_remote_copy(
            src_ref=src, dst_ref=dst, send_sem=send, recv_sem=recv, device_id=where, device_id_type=MESH
        )

    barrier = pltpu.get_barrier_semaphore()
    count = 0
    for k in range(1, n_section):
        pl.semaphore_signal(
            barrier, inc=1, device_id={"section": lax.rem(sec + k, n_section)}, device_id_type=MESH
        )
        count += 1
    if scatter:
        pl.semaphore_signal(barrier, inc=1, device_id={"dp": mate}, device_id_type=MESH)
        count += 1
        for k in range(1, pairs):
            other = lax.rem(place + k, pairs) * 2 + core
            pl.semaphore_signal(barrier, inc=1, device_id={"dp": other}, device_id_type=MESH)
            count += 1

    mirror = n_section - 1 - sec
    below = lax.max(sec - 1, 0)
    values = [remote(ybuf.at[m], zbuf.at[m], vs.at[m], vr.at[m], section=mirror) for m in range(n_micro)]
    chains = [remote(cbuf.at[m], gbuf.at[m], cs.at[m], cr.at[m], section=below) for m in range(n_micro)]
    skips = [remote(kbuf.at[m], skbuf.at[m], ks.at[m], kr.at[m], section=mirror) for m in range(n_micro)]

    def forward(m):
        span = slice(m * rows, (m + 1) * rows)
        side = zbuf[m]
        zall[:, span] = side
        united = x[0, m].astype(F32) + jnp.dot(wsk_t[...], side, preferred_element_type=F32)
        recip = lax.rsqrt(jnp.mean(united * united, axis=0, keepdims=True) + EPS)
        normed = (united * recip).astype(BF16)
        preact = jnp.dot(win_n[...], normed, preferred_element_type=F32)
        sigma = jax.nn.sigmoid(preact)
        active = (preact * sigma).astype(BF16)
        ubuf[m] = united
        rbuf[m] = recip
        nbuf[:, span] = normed
        abuf[:, span] = active
        dbuf[m] = sigma * (1.0 + preact * (1.0 - sigma))
        return united, active

    wsk_t[...] = w_skip[0].T
    win_n[...] = w_in[0].T

    @pl.when(sec < half)
    def _():
        levels = lax.broadcasted_iota(jnp.int32, (table.shape[1], rows), 0)
        for m in range(n_micro):
            onehot = (levels == ts[m : m + 1, :]).astype(F32).astype(BF16)
            zbuf[m] = jnp.dot(table[...], onehot, preferred_element_type=F32).astype(BF16)
            united, active = forward(m)
            output = united + jnp.dot(w_out[0], active, preferred_element_type=F32)
            ybuf[m] = output.astype(BF16)
            if m == 0:
                pl.semaphore_wait(barrier, count)
            values[m].start()

    wout_n[...] = w_out[0].T

    @pl.when(sec >= half - 1)
    def _():
        skbuf[...] = jnp.zeros_like(skbuf)

    @pl.when(sec >= half)
    def _():
        pl.semaphore_wait(barrier, count)

    for m in range(n_micro):

        @pl.when(sec >= half)
        def _():
            values[m].wait_recv()
            forward(m)

        @pl.when(sec == n_section - 1)
        def _():
            gbuf[m] = cot[m]

        @pl.when(sec < n_section - 1)
        def _():
            chains[m].wait_recv()

        @pl.when(sec < half - 1)
        def _():
            skips[m].wait_recv()

        span = slice(m * rows, (m + 1) * rows)
        grad_out = gbuf[m].astype(F32) + skbuf[m].astype(F32)
        grad_low = grad_out.astype(BF16)
        lowbuf[:, span] = grad_low
        grad_act = jnp.dot(wout_n[...], grad_low, preferred_element_type=F32)
        grad_pre = (grad_act * dbuf[m]).astype(BF16)
        gpbuf[:, span] = grad_pre
        grad_norm = jnp.dot(w_in[0], grad_pre, preferred_element_type=F32)
        united = ubuf[m]
        recip = rbuf[m]
        grad_united = (
            grad_out
            + recip * grad_norm
            - united * recip**3 * jnp.mean(grad_norm * united, axis=0, keepdims=True)
        )
        low = grad_united.astype(BF16)

        @pl.when(sec != half)
        def _():
            cbuf[m] = low

            @pl.when(sec > 0)
            def _():
                chains[m].start()

        @pl.when(sec >= half)
        def _():
            back = jnp.dot(w_skip[0], low, preferred_element_type=F32).astype(BF16)

            @pl.when(sec == half)
            def _():
                cbuf[m] = (low.astype(F32) + back.astype(F32)).astype(BF16)
                chains[m].start()

            @pl.when(sec > half)
            def _():
                kbuf[m] = back
                skips[m].start()

        ig[0, m] = low
        gall[:, span] = low

    def product(left, right):
        return contract(left, right, ((1,), (1,)))

    if scatter:
        (acc, pbuf, precv, tot, sbuf_r, sbuf_l, in_r, in_l, ps, pr, rss, rsr, lss, lsr) = rs
        fh = hidden // n_dp
        kh = width // n_dp
        full = width // LANES
        tail = width % LANES
        stack = acc.shape[1]
        piece = stack // CHUNKS
        mix = 2 * full * fh
        order = []
        for t in range(pairs):
            k = pairs - 1 - t // 2 if t % 2 == 0 else t // 2
            order.append(k)
        first = [
            remote(pbuf.at[t], precv.at[t], ps.at[t], pr.at[t], dp=mate) for t in range(pairs)
        ]
        for t in order:
            fspan = slice(2 * t * fh, 2 * (t + 1) * fh)
            kspan = slice(2 * t * kh, 2 * (t + 1) * kh)
            d_out = product(abuf[fspan, :], lowbuf[...])
            d_in = product(gpbuf[fspan, :], nbuf[...])
            d_skip = product(zall[kspan, :], gall[...])
            for c in range(2):
                d = 2 * t + c
                for i in range(full):
                    cut = slice(i * LANES, (i + 1) * LANES)
                    acc[d, i * fh : (i + 1) * fh, :] = d_in[c * fh : (c + 1) * fh, cut]
                    acc[d, (full + i) * fh : (full + i + 1) * fh, :] = d_out[c * fh : (c + 1) * fh, cut]
                    at = mix + fh + i * kh
                    acc[d, at : at + kh, :] = d_skip[c * kh : (c + 1) * kh, cut]
                rest = slice(full * LANES, width)
                acc[d, mix : mix + fh, 0:tail] = d_in[c * fh : (c + 1) * fh, rest]
                acc[d, mix : mix + fh, tail : 2 * tail] = d_out[c * fh : (c + 1) * fh, rest]
                at = mix + fh + full * kh
                acc[d, at:stack, :] = jnp.zeros((stack - at, LANES), F32)
                acc[d, at : at + kh, 0:tail] = d_skip[c * kh : (c + 1) * kh, rest]
            pbuf[t] = acc[2 * t + 1 - core].astype(BF16)
            first[t].start()

        def hop(sbuf, into, send, recv, t, q, step):
            rows_of = pl.ds(q * piece, piece)
            at = jnp.clip(place + step, 0, pairs - 1) * 2 + core
            return remote(
                sbuf.at[t, rows_of], into.at[t, rows_of], send.at[t, q], recv.at[t, q], dp=at
            )

        def right(t, q):
            return hop(sbuf_r, in_r, rss, rsr, t, q, 1)

        def left(t, q):
            return hop(sbuf_l, in_l, lss, lsr, t, q, -1)

        for t in order:
            first[t].wait_recv()
            tot[t] = acc[2 * t + core] + precv[t].astype(F32)

        def push(copy, into, sbuf, t, inner):
            for q in range(CHUNKS):
                rows_of = pl.ds(q * piece, piece)

                @pl.when(inner)
                def _():
                    copy(t, q).wait_recv()
                    sbuf[t, rows_of] = (tot[t, rows_of] + into[t, rows_of].astype(F32)).astype(BF16)

                @pl.when(jnp.logical_not(inner))
                def _():
                    sbuf[t, rows_of] = tot[t, rows_of].astype(BF16)

                copy(t, q).start()

        def push_right(t):
            @pl.when(place < t)
            def _():
                push(right, in_r, sbuf_r, t, place > 0)

        def push_left(t):
            @pl.when(place > t)
            def _():
                push(left, in_l, sbuf_l, t, place < pairs - 1)

        for j in range(pairs - 1):

            @pl.when(2 * place < pairs)
            def _():
                push_right(pairs - 1 - j)
                push_left(j)

            @pl.when(2 * place >= pairs)
            def _():
                push_left(j)
                push_right(pairs - 1 - j)

        for q in range(CHUNKS):
            rows_of = pl.ds(q * piece, piece)

            @pl.when(place > 0)
            def _():
                right(place, q).wait_recv()
                tot[place, rows_of] += in_r[place, rows_of].astype(F32)

            @pl.when(place < pairs - 1)
            def _():
                left(place, q).wait_recv()
                tot[place, rows_of] += in_l[place, rows_of].astype(F32)

        for i in range(full):
            cut = slice(i * LANES, (i + 1) * LANES)
            g_in[:, cut] = tot[place, i * fh : (i + 1) * fh, :]
            g_out[:, cut] = tot[place, (full + i) * fh : (full + i + 1) * fh, :]
            at = mix + fh + i * kh
            g_skip[:, cut] = tot[place, at : at + kh, :]
        rest = slice(full * LANES, width)
        at = mix + fh + full * kh
        g_in[:, rest] = tot[place, mix : mix + fh, 0:tail]
        g_out[:, rest] = tot[place, mix : mix + fh, tail : 2 * tail]
        g_skip[:, rest] = tot[place, at : at + kh, 0:tail]
        for t in range(pairs):
            first[t].wait_send()

            @pl.when(place < t)
            def _():
                for q in range(CHUNKS):
                    right(t, q).wait_send()

            @pl.when(place > t)
            def _():
                for q in range(CHUNKS):
                    left(t, q).wait_send()
    else:
        g_in[...] = product(gpbuf[...], nbuf[...])
        g_out[...] = product(abuf[...], lowbuf[...])
        g_skip[...] = product(zall[...], gall[...])

    for m in range(n_micro):

        @pl.when(sec < half)
        def _():
            values[m].wait_send()

        @pl.when(sec > 0)
        def _():
            chains[m].wait_send()

        @pl.when(sec > half)
        def _():
            skips[m].wait_send()


def shards(n_section, n_dp, saved_inputs, timesteps, time_table, skip_weight, ff_in, ff_out, output_cotangent):
    n_micro, rows, width = output_cotangent.shape
    hidden = ff_in.shape[1]
    pairs = n_dp // 2
    aligned = hidden % (16 * n_dp) == 0 and width % (8 * n_dp) == 0
    scatter = n_dp % 2 == 0 and aligned and width % LANES == LANES // 2
    fh = hidden // n_dp if scatter else hidden
    kh = width // n_dp if scatter else width
    every = n_micro * rows
    low = pltpu.VMEM((n_micro, width, rows), BF16)
    wide = pltpu.VMEM((width, every), BF16)
    scratch = [
        pltpu.VMEM((width, width), BF16),
        pltpu.VMEM((hidden, width), BF16),
        pltpu.VMEM((hidden, width), BF16),
        low,
        wide,
        low,
        pltpu.VMEM((n_micro, width, rows), F32),
        pltpu.VMEM((n_micro, 1, rows), F32),
        wide,
        pltpu.VMEM((hidden, every), BF16),
        pltpu.VMEM((n_micro, hidden, rows), F32),
        low,
        wide,
        pltpu.VMEM((hidden, every), BF16),
        wide,
        low,
        low,
        low,
    ] + [pltpu.SemaphoreType.DMA((n_micro,))] * 6
    if scatter:
        full = width // LANES
        stack = (2 * full + 1) * fh + (full + 1) * kh
        stack = -(-stack // (16 * CHUNKS)) * 16 * CHUNKS
        block = pltpu.VMEM((pairs, stack, LANES), BF16)
        scratch += [pltpu.VMEM((n_dp, stack, LANES), F32), block, block]
        scratch += [pltpu.VMEM((pairs, stack, LANES), F32), block, block, block, block]
        scratch += [pltpu.SemaphoreType.DMA((pairs,))] * 2
        scratch += [pltpu.SemaphoreType.DMA((pairs, CHUNKS))] * 4
    turned = (
        jnp.swapaxes(saved_inputs, 2, 3),
        timesteps,
        time_table.T,
        skip_weight,
        jnp.swapaxes(ff_in, 1, 2),
        jnp.swapaxes(ff_out, 1, 2),
        jnp.swapaxes(output_cotangent, 1, 2),
    )
    grad_store, grad_skip, grad_in, grad_out = pl.pallas_call(
        functools.partial(kernel, n_section, n_dp, scatter),
        out_shape=(
            jax.ShapeDtypeStruct(turned[0].shape, BF16),
            jax.ShapeDtypeStruct((kh, width), F32),
            jax.ShapeDtypeStruct((fh, width), F32),
            jax.ShapeDtypeStruct((fh, width), F32),
        ),
        in_specs=[pl.BlockSpec(memory_space=pltpu.VMEM)] * 7,
        out_specs=[pl.BlockSpec(memory_space=pltpu.VMEM)] * 4,
        scratch_shapes=scratch,
        compiler_params=pltpu.CompilerParams(
            collective_id=0, has_side_effects=True, vmem_limit_bytes=60 * 1024 * 1024
        ),
    )(*turned)
    grad_store = jnp.swapaxes(grad_store, 2, 3)
    grad_skip = grad_skip.reshape(-1)
    if not scatter:
        grad_in, grad_out, grad_skip = (
            lax.psum_scatter(value, "dp", scatter_dimension=0, tiled=True)
            for value in (grad_in, grad_out, grad_skip)
        )
    return (grad_store, grad_skip[None], grad_in[None], grad_out[None])


def solution(mesh):
    in_specs = (
        P("section", None, "dp", None),
        P(None, "dp"),
        P(),
        P("section", None, None),
        P("section", None, None),
        P("section", None, None),
        P(None, "dp", None),
    )
    out_specs = (
        P("section", None, "dp", None),
        P("section", "dp"),
        P("section", "dp", None),
        P("section", "dp", None),
    )
    body = functools.partial(shards, mesh.shape["section"], mesh.shape["dp"])
    return jax.shard_map(body, mesh=mesh, in_specs=in_specs, out_specs=out_specs, check_vma=False)
```

```python
import functools

import jax
import jax.numpy as jnp
from jax import lax
from jax.experimental import pallas as pl
from jax.experimental.pallas import tpu as pltpu
from jax.sharding import PartitionSpec as P

EPS = 1e-06
MESH = pl.DeviceIdType.MESH
F32 = jnp.float32
BF16 = jnp.bfloat16
LANES = 128


def contract(left, right, dims):
    return lax.dot_general(
        left, right, ((dims[0], dims[1]), ((), ())), preferred_element_type=jnp.float32
    )


def kernel(n_section, n_dp, scatter, *refs):
    (x, ts, table, w_skip, w_in, w_out, cot) = refs[:7]
    (ig, g_out, g_in, g_skip) = refs[7:11]
    (wsk_t, win_n, wout_n, zbuf, zall, ybuf, ubuf, rbuf, nbuf, abuf, dbuf) = refs[11:22]
    (gbuf, lowbuf, gpbuf, gall, cbuf, kbuf, skbuf) = refs[22:29]
    (vs, vr, cs, cr, ks, kr) = refs[29:35]
    rs = refs[35:]
    sec = lax.axis_index("section")
    dp = lax.axis_index("dp")
    n_micro, width, rows = cot.shape
    hidden = w_in.shape[2]
    half = n_section // 2
    pairs = n_dp // 2
    core = lax.rem(dp, 2)
    place = lax.div(dp, 2)
    mate = dp + 1 - 2 * core

    def remote(src, dst, send, recv, **where):
        return pltpu.make_async_remote_copy(
            src_ref=src, dst_ref=dst, send_sem=send, recv_sem=recv, device_id=where, device_id_type=MESH
        )

    barrier = pltpu.get_barrier_semaphore()
    count = 0
    for k in range(1, n_section):
        pl.semaphore_signal(
            barrier, inc=1, device_id={"section": lax.rem(sec + k, n_section)}, device_id_type=MESH
        )
        count += 1
    if scatter:
        pl.semaphore_signal(barrier, inc=1, device_id={"dp": mate}, device_id_type=MESH)
        count += 1
        for k in range(1, pairs):
            other = lax.rem(place + k, pairs) * 2 + core
            pl.semaphore_signal(barrier, inc=1, device_id={"dp": other}, device_id_type=MESH)
            count += 1

    mirror = n_section - 1 - sec
    below = lax.max(sec - 1, 0)
    values = [remote(ybuf.at[m], zbuf.at[m], vs.at[m], vr.at[m], section=mirror) for m in range(n_micro)]
    chains = [remote(cbuf.at[m], gbuf.at[m], cs.at[m], cr.at[m], section=below) for m in range(n_micro)]
    skips = [remote(kbuf.at[m], skbuf.at[m], ks.at[m], kr.at[m], section=mirror) for m in range(n_micro)]

    def forward(m):
        span = slice(m * rows, (m + 1) * rows)
        side = zbuf[m]
        zall[:, span] = side
        united = x[0, m].astype(F32) + jnp.dot(wsk_t[...], side, preferred_element_type=F32)
        recip = lax.rsqrt(jnp.mean(united * united, axis=0, keepdims=True) + EPS)
        normed = (united * recip).astype(BF16)
        preact = jnp.dot(win_n[...], normed, preferred_element_type=F32)
        sigma = jax.nn.sigmoid(preact)
        active = (preact * sigma).astype(BF16)
        ubuf[m] = united
        rbuf[m] = recip
        nbuf[:, span] = normed
        abuf[:, span] = active
        dbuf[m] = sigma * (1.0 + preact * (1.0 - sigma))
        return united, active

    wsk_t[...] = w_skip[0].T
    win_n[...] = w_in[0].T

    @pl.when(sec < half)
    def _():
        levels = lax.broadcasted_iota(jnp.int32, (table.shape[1], rows), 0)
        for m in range(n_micro):
            onehot = (levels == ts[m : m + 1, :]).astype(F32).astype(BF16)
            zbuf[m] = jnp.dot(table[...], onehot, preferred_element_type=F32).astype(BF16)
            united, active = forward(m)
            output = united + jnp.dot(w_out[0], active, preferred_element_type=F32)
            ybuf[m] = output.astype(BF16)
            if m == 0:
                pl.semaphore_wait(barrier, count)
            values[m].start()

    wout_n[...] = w_out[0].T

    @pl.when(sec >= half - 1)
    def _():
        skbuf[...] = jnp.zeros_like(skbuf)

    @pl.when(sec >= half)
    def _():
        pl.semaphore_wait(barrier, count)

    def product(left, right):
        return contract(left, right, ((1,), (1,)))

    if scatter:
        parts = [rs[8 * p : 8 * p + 8] for p in range(3)]
        (ps, pr, rss, rsr, lss, lsr) = rs[24:]
        full = width // LANES
        tail = width % LANES
        factors = ((abuf, lowbuf, hidden // n_dp), (gpbuf, nbuf, hidden // n_dp), (zall, gall, width // n_dp))
        order = [pairs - 1 - t // 2 if t % 2 == 0 else t // 2 for t in range(pairs)]
        ends = (place == 0) | (place == pairs - 1)

        def first(p, t):
            return remote(parts[p][1].at[t], parts[p][2].at[t], ps.at[p, t], pr.at[p, t], dp=mate)

        def products(p):
            (acc, pbuf) = parts[p][:2]
            (left_ref, right_ref, n) = factors[p]
            used = full * n + n // 2
            for t in order:
                block = product(left_ref[2 * t * n : 2 * (t + 1) * n, :], right_ref[...])
                for k in range(2):
                    own = block[k * n : (k + 1) * n]
                    for i in range(full):
                        acc[2 * t + k, i * n : (i + 1) * n, :] = own[:, i * LANES : (i + 1) * LANES]
                    acc[2 * t + k, full * n : used, 0:tail] = own[0 : n // 2, full * LANES :]
                    acc[2 * t + k, full * n : used, tail:] = own[n // 2 :, full * LANES :]
                    if acc.shape[1] > used:
                        acc[2 * t + k, used:, :] = jnp.zeros((acc.shape[1] - used, LANES), F32)
                pbuf[t] = acc[2 * t + 1 - core].astype(BF16)
                first(p, t).start()

        def hop(sbuf, into, send, recv, p, t, step):
            at = jnp.clip(place + step, 0, pairs - 1) * 2 + core
            return remote(sbuf.at[t], into.at[t], send.at[p, t], recv.at[p, t], dp=at)

        def right(p, t):
            return hop(parts[p][4], parts[p][6], rss, rsr, p, t, 1)

        def left(p, t):
            return hop(parts[p][5], parts[p][7], lss, lsr, p, t, -1)

        def meet(p):
            for t in order:
                first(p, t).wait_recv()
                parts[p][3][t] = parts[p][0][2 * t + core] + parts[p][2][t].astype(F32)

        def push(copy, sbuf, into, total, p, t, inner):
            @pl.when(inner)
            def _():
                copy(p, t).wait_recv()
                sbuf[t] = (total[t] + into[t].astype(F32)).astype(BF16)

            @pl.when(jnp.logical_not(inner))
            def _():
                sbuf[t] = total[t].astype(BF16)

            copy(p, t).start()

        def push_right(group, t):
            @pl.when(place < t)
            def _():
                for p in group:
                    push(right, parts[p][4], parts[p][6], parts[p][3], p, t, place > 0)

        def push_left(group, t):
            @pl.when(place > t)
            def _():
                for p in group:
                    push(left, parts[p][5], parts[p][7], parts[p][3], p, t, place < pairs - 1)

        def line(group):
            for p in group:
                meet(p)
            for j in range(pairs - 1):

                @pl.when(2 * place < pairs)
                def _():
                    push_right(group, pairs - 1 - j)
                    push_left(group, j)

                @pl.when(2 * place >= pairs)
                def _():
                    push_left(group, j)
                    push_right(group, pairs - 1 - j)

    for m in range(n_micro):

        @pl.when(sec >= half)
        def _():
            values[m].wait_recv()
            forward(m)

        @pl.when(sec == n_section - 1)
        def _():
            gbuf[m] = cot[m]

        @pl.when(sec < n_section - 1)
        def _():
            chains[m].wait_recv()

        @pl.when(sec < half - 1)
        def _():
            skips[m].wait_recv()

        span = slice(m * rows, (m + 1) * rows)
        grad_out = gbuf[m].astype(F32) + skbuf[m].astype(F32)
        grad_low = grad_out.astype(BF16)
        lowbuf[:, span] = grad_low
        if scatter and m == n_micro - 1:

            @pl.when(sec == 0)
            def _():
                products(0)

                @pl.when(ends)
                def _():
                    line((0,))

        grad_act = jnp.dot(wout_n[...], grad_low, preferred_element_type=F32)
        grad_pre = (grad_act * dbuf[m]).astype(BF16)
        gpbuf[:, span] = grad_pre
        grad_norm = jnp.dot(w_in[0], grad_pre, preferred_element_type=F32)
        united = ubuf[m]
        recip = rbuf[m]
        grad_united = (
            grad_out
            + recip * grad_norm
            - united * recip**3 * jnp.mean(grad_norm * united, axis=0, keepdims=True)
        )
        low = grad_united.astype(BF16)

        @pl.when(sec != half)
        def _():
            cbuf[m] = low

            @pl.when(sec > 0)
            def _():
                chains[m].start()

        @pl.when(sec >= half)
        def _():
            back = jnp.dot(w_skip[0], low, preferred_element_type=F32).astype(BF16)

            @pl.when(sec == half)
            def _():
                cbuf[m] = (low.astype(F32) + back.astype(F32)).astype(BF16)
                chains[m].start()

            @pl.when(sec > half)
            def _():
                kbuf[m] = back
                skips[m].start()

        ig[0, m] = low
        gall[:, span] = low

    if scatter:

        @pl.when(sec > 0)
        def _():
            products(0)

        products(1)
        products(2)

        @pl.when((sec > 0) | jnp.logical_not(ends))
        def _():
            line((0,))

        line((1, 2))
        for p, result in enumerate((g_out, g_in, g_skip)):
            total = parts[p][3]

            @pl.when(place > 0)
            def _():
                right(p, place).wait_recv()
                total[place] += parts[p][6][place].astype(F32)

            @pl.when(place < pairs - 1)
            def _():
                left(p, place).wait_recv()
                total[place] += parts[p][7][place].astype(F32)

            result[...] = total[place]
            for t in range(pairs):
                first(p, t).wait_send()

                @pl.when(place < t)
                def _():
                    right(p, t).wait_send()

                @pl.when(place > t)
                def _():
                    left(p, t).wait_send()
    else:
        g_in[...] = product(gpbuf[...], nbuf[...])
        g_out[...] = product(abuf[...], lowbuf[...])
        g_skip[...] = product(zall[...], gall[...])

    for m in range(n_micro):

        @pl.when(sec < half)
        def _():
            values[m].wait_send()

        @pl.when(sec > 0)
        def _():
            chains[m].wait_send()

        @pl.when(sec > half)
        def _():
            skips[m].wait_send()


def finish(ig, p_out, p_in, p_skip, o_ig, o_skip, o_in, o_out, flat):
    o_ig[...] = ig[...]
    for packed, result in ((p_out, o_out), (p_in, o_in), (p_skip, flat)):
        (n, width) = result.shape
        full = width // LANES
        tail = width % LANES
        for i in range(full):
            result[:, i * LANES : (i + 1) * LANES] = packed[i * n : (i + 1) * n, :]
        used = full * n + n // 2
        result[0 : n // 2, full * LANES :] = packed[full * n : used, 0:tail]
        result[n // 2 :, full * LANES :] = packed[full * n : used, tail:]
    (n, width) = flat.shape
    for r in range(n):
        o_skip[:, r * width : (r + 1) * width] = flat[r : r + 1, :]


def shards(n_section, n_dp, saved_inputs, timesteps, time_table, skip_weight, ff_in, ff_out, output_cotangent):
    n_micro, rows, width = output_cotangent.shape
    hidden = ff_in.shape[1]
    pairs = n_dp // 2
    aligned = hidden % (16 * n_dp) == 0 and width % (8 * n_dp) == 0
    scatter = n_dp % 2 == 0 and aligned and width % LANES == LANES // 2
    fh = hidden // n_dp if scatter else hidden
    kh = width // n_dp if scatter else width
    every = n_micro * rows
    low = pltpu.VMEM((n_micro, width, rows), BF16)
    wide = pltpu.VMEM((width, every), BF16)
    scratch = [
        pltpu.VMEM((width, width), BF16),
        pltpu.VMEM((hidden, width), BF16),
        pltpu.VMEM((hidden, width), BF16),
        low,
        wide,
        low,
        pltpu.VMEM((n_micro, width, rows), F32),
        pltpu.VMEM((n_micro, 1, rows), F32),
        wide,
        pltpu.VMEM((hidden, every), BF16),
        pltpu.VMEM((n_micro, hidden, rows), F32),
        low,
        wide,
        pltpu.VMEM((hidden, every), BF16),
        wide,
        low,
        low,
        low,
    ] + [pltpu.SemaphoreType.DMA((n_micro,))] * 6
    sums = ((fh, width), (fh, width), (kh, width))
    if scatter:
        full = width // LANES
        sums = tuple((-(-(full * n + n // 2) // 16) * 16, LANES) for n in (fh, fh, kh))
        for n, lanes in sums:
            block = pltpu.VMEM((pairs, n, lanes), BF16)
            scratch += [pltpu.VMEM((n_dp, n, lanes), F32), block, block]
            scratch += [pltpu.VMEM((pairs, n, lanes), F32), block, block, block, block]
        scratch += [pltpu.SemaphoreType.DMA((3, pairs))] * 6
    turned = (
        jnp.swapaxes(saved_inputs, 2, 3),
        timesteps,
        time_table.T,
        skip_weight,
        jnp.swapaxes(ff_in, 1, 2),
        jnp.swapaxes(ff_out, 1, 2),
        jnp.swapaxes(output_cotangent, 1, 2),
    )
    vmem = pl.BlockSpec(memory_space=pltpu.VMEM)
    store_shape = jax.ShapeDtypeStruct(turned[0].shape, BF16)
    grad_store, grad_out, grad_in, grad_skip = pl.pallas_call(
        functools.partial(kernel, n_section, n_dp, scatter),
        out_shape=(store_shape,) + tuple(jax.ShapeDtypeStruct(shape, F32) for shape in sums),
        in_specs=[vmem] * 7,
        out_specs=[vmem] * 4,
        scratch_shapes=scratch,
        compiler_params=pltpu.CompilerParams(
            collective_id=0, has_side_effects=True, vmem_limit_bytes=44 * 1024 * 1024
        ),
    )(*turned)
    if scatter:
        grad_store, grad_skip, grad_in, grad_out = pl.pallas_call(
            finish,
            out_shape=(
                store_shape,
                jax.ShapeDtypeStruct((1, kh * width), F32),
                jax.ShapeDtypeStruct((fh, width), F32),
                jax.ShapeDtypeStruct((fh, width), F32),
            ),
            in_specs=[vmem] * 4,
            out_specs=[vmem] * 4,
            scratch_shapes=[pltpu.VMEM((kh, width), F32)],
            compiler_params=pltpu.CompilerParams(vmem_limit_bytes=8 * 1024 * 1024),
        )(grad_store, grad_out, grad_in, grad_skip)
    else:
        grad_in, grad_out, grad_skip = (
            lax.psum_scatter(value, "dp", scatter_dimension=0, tiled=True)
            for value in (grad_in, grad_out, grad_skip.reshape(-1))
        )
        grad_skip = grad_skip[None]
    grad_store = jnp.swapaxes(grad_store, 2, 3)
    return (grad_store, grad_skip, grad_in[None], grad_out[None])


def solution(mesh):
    in_specs = (
        P("section", None, "dp", None),
        P(None, "dp"),
        P(),
        P("section", None, None),
        P("section", None, None),
        P("section", None, None),
        P(None, "dp", None),
    )
    out_specs = (
        P("section", None, "dp", None),
        P("section", "dp"),
        P("section", "dp", None),
        P("section", "dp", None),
    )
    body = functools.partial(shards, mesh.shape["section"], mesh.shape["dp"])
    return jax.shard_map(body, mesh=mesh, in_specs=in_specs, out_specs=out_specs, check_vma=False)
```

```python
import functools

import jax
import jax.numpy as jnp
from jax import lax
from jax.experimental import pallas as pl
from jax.experimental.pallas import tpu as pltpu
from jax.sharding import PartitionSpec as P

EPS = 1e-06
MESH = pl.DeviceIdType.MESH
F32 = jnp.float32
BF16 = jnp.bfloat16
LANES = 128
CHUNKS = 2


def contract(left, right, dims):
    return lax.dot_general(
        left, right, ((dims[0], dims[1]), ((), ())), preferred_element_type=jnp.float32
    )


def kernel(n_section, n_dp, scatter, *refs):
    outside = refs[:7]
    results = 2 if scatter else 4
    ig = refs[7]
    sums = refs[8 : 7 + results]
    refs = refs[:11] + refs[7 + results :]
    (wsk_t, win_n, wout_n, zbuf, zall, ybuf, ubuf, rbuf, nbuf, abuf, dbuf) = refs[11:22]
    (gbuf, lowbuf, gpbuf, gall, cbuf, kbuf, skbuf) = refs[22:29]
    (vs, vr, cs, cr, ks, kr) = refs[29:35]
    inside = refs[35:42]
    (x, ts, table, w_skip, w_in, w_out, cot) = inside
    loaded = refs[42]
    rs = refs[43:]
    loads = [pltpu.make_async_copy(outside[i], inside[i], loaded.at[i]) for i in range(7)]
    for i in (3, 4, 1, 2, 0, 5, 6):
        loads[i].start()
    sec = lax.axis_index("section")
    dp = lax.axis_index("dp")
    n_micro, width, rows = cot.shape
    hidden = w_in.shape[2]
    half = n_section // 2
    pairs = n_dp // 2
    core = lax.rem(dp, 2)
    place = lax.div(dp, 2)
    mate = dp + 1 - 2 * core

    def remote(src, dst, send, recv, **where):
        return pltpu.make_async_remote_copy(
            src_ref=src, dst_ref=dst, send_sem=send, recv_sem=recv, device_id=where, device_id_type=MESH
        )

    barrier = pltpu.get_barrier_semaphore()
    count = 0
    for k in range(1, n_section):
        pl.semaphore_signal(
            barrier, inc=1, device_id={"section": lax.rem(sec + k, n_section)}, device_id_type=MESH
        )
        count += 1
    if scatter:
        pl.semaphore_signal(barrier, inc=1, device_id={"dp": mate}, device_id_type=MESH)
        count += 1
        for k in range(1, pairs):
            other = lax.rem(place + k, pairs) * 2 + core
            pl.semaphore_signal(barrier, inc=1, device_id={"dp": other}, device_id_type=MESH)
            count += 1

    mirror = n_section - 1 - sec
    below = lax.max(sec - 1, 0)
    values = [remote(ybuf.at[m], zbuf.at[m], vs.at[m], vr.at[m], section=mirror) for m in range(n_micro)]
    chains = [remote(cbuf.at[m], gbuf.at[m], cs.at[m], cr.at[m], section=below) for m in range(n_micro)]
    skips = [remote(kbuf.at[m], skbuf.at[m], ks.at[m], kr.at[m], section=mirror) for m in range(n_micro)]

    def forward(m):
        span = slice(m * rows, (m + 1) * rows)
        side = zbuf[m]
        zall[:, span] = side
        united = x[0, m].astype(F32) + jnp.dot(wsk_t[...], side, preferred_element_type=F32)
        recip = lax.rsqrt(jnp.mean(united * united, axis=0, keepdims=True) + EPS)
        normed = (united * recip).astype(BF16)
        preact = jnp.dot(win_n[...], normed, preferred_element_type=F32)
        sigma = jax.nn.sigmoid(preact)
        active = (preact * sigma).astype(BF16)
        ubuf[m] = united
        rbuf[m] = recip
        nbuf[:, span] = normed
        abuf[:, span] = active
        dbuf[m] = sigma * (1.0 + preact * (1.0 - sigma))
        return united, active

    loads[3].wait()
    wsk_t[...] = w_skip[0].T
    loads[4].wait()
    win_n[...] = w_in[0].T
    for i in (1, 2, 0, 5):
        loads[i].wait()

    @pl.when(sec < half)
    def _():
        levels = lax.broadcasted_iota(jnp.int32, (table.shape[1], rows), 0)
        for m in range(n_micro):
            onehot = (levels == ts[m : m + 1, :]).astype(F32).astype(BF16)
            zbuf[m] = jnp.dot(table[...], onehot, preferred_element_type=F32).astype(BF16)
            united, active = forward(m)
            output = united + jnp.dot(w_out[0], active, preferred_element_type=F32)
            ybuf[m] = output.astype(BF16)
            if m == 0:
                pl.semaphore_wait(barrier, count)
            values[m].start()

    wout_n[...] = w_out[0].T
    loads[6].wait()

    @pl.when(sec >= half - 1)
    def _():
        skbuf[...] = jnp.zeros_like(skbuf)

    @pl.when(sec >= half)
    def _():
        pl.semaphore_wait(barrier, count)

    for m in range(n_micro):

        @pl.when(sec >= half)
        def _():
            values[m].wait_recv()
            forward(m)

        @pl.when(sec == n_section - 1)
        def _():
            gbuf[m] = cot[m]

        @pl.when(sec < n_section - 1)
        def _():
            chains[m].wait_recv()

        @pl.when(sec < half - 1)
        def _():
            skips[m].wait_recv()

        span = slice(m * rows, (m + 1) * rows)
        grad_out = gbuf[m].astype(F32) + skbuf[m].astype(F32)
        grad_low = grad_out.astype(BF16)
        lowbuf[:, span] = grad_low
        grad_act = jnp.dot(wout_n[...], grad_low, preferred_element_type=F32)
        grad_pre = (grad_act * dbuf[m]).astype(BF16)
        gpbuf[:, span] = grad_pre
        grad_norm = jnp.dot(w_in[0], grad_pre, preferred_element_type=F32)
        united = ubuf[m]
        recip = rbuf[m]
        grad_united = (
            grad_out
            + recip * grad_norm
            - united * recip**3 * jnp.mean(grad_norm * united, axis=0, keepdims=True)
        )
        low = grad_united.astype(BF16)

        @pl.when(sec != half)
        def _():
            cbuf[m] = low

            @pl.when(sec > 0)
            def _():
                chains[m].start()

        @pl.when(sec >= half)
        def _():
            back = jnp.dot(w_skip[0], low, preferred_element_type=F32).astype(BF16)

            @pl.when(sec == half)
            def _():
                cbuf[m] = (low.astype(F32) + back.astype(F32)).astype(BF16)
                chains[m].start()

            @pl.when(sec > half)
            def _():
                kbuf[m] = back
                skips[m].start()

        ig[0, m] = low
        gall[:, span] = low

    def product(left, right):
        return contract(left, right, ((1,), (1,)))

    if scatter:
        (acc, pbuf, precv, tot, sbuf_r, sbuf_l, in_r, in_l, ps, pr, rss, rsr, lss, lsr) = rs
        fh = hidden // n_dp
        kh = width // n_dp
        full = width // LANES
        tail = width % LANES
        stack = acc.shape[1]
        piece = stack // CHUNKS
        mix = 2 * full * fh
        order = []
        for t in range(pairs):
            k = pairs - 1 - t // 2 if t % 2 == 0 else t // 2
            order.append(k)
        first = [
            remote(pbuf.at[t], precv.at[t], ps.at[t], pr.at[t], dp=mate) for t in range(pairs)
        ]
        for t in order:
            fspan = slice(2 * t * fh, 2 * (t + 1) * fh)
            kspan = slice(2 * t * kh, 2 * (t + 1) * kh)
            d_out = product(abuf[fspan, :], lowbuf[...])
            d_in = product(gpbuf[fspan, :], nbuf[...])
            d_skip = product(zall[kspan, :], gall[...])
            for c in range(2):
                d = 2 * t + c
                for i in range(full):
                    cut = slice(i * LANES, (i + 1) * LANES)
                    acc[d, i * fh : (i + 1) * fh, :] = d_in[c * fh : (c + 1) * fh, cut]
                    acc[d, (full + i) * fh : (full + i + 1) * fh, :] = d_out[c * fh : (c + 1) * fh, cut]
                    at = mix + fh + i * kh
                    acc[d, at : at + kh, :] = d_skip[c * kh : (c + 1) * kh, cut]
                rest = slice(full * LANES, width)
                acc[d, mix : mix + fh, 0:tail] = d_in[c * fh : (c + 1) * fh, rest]
                acc[d, mix : mix + fh, tail : 2 * tail] = d_out[c * fh : (c + 1) * fh, rest]
                at = mix + fh + full * kh
                acc[d, at:stack, :] = jnp.zeros((stack - at, LANES), F32)
                acc[d, at : at + kh, 0:tail] = d_skip[c * kh : (c + 1) * kh, rest]
            pbuf[t] = acc[2 * t + 1 - core].astype(BF16)
            first[t].start()

        def hop(sbuf, into, send, recv, t, q, step):
            rows_of = pl.ds(q * piece, piece)
            at = jnp.clip(place + step, 0, pairs - 1) * 2 + core
            return remote(
                sbuf.at[t, rows_of], into.at[t, rows_of], send.at[t, q], recv.at[t, q], dp=at
            )

        def right(t, q):
            return hop(sbuf_r, in_r, rss, rsr, t, q, 1)

        def left(t, q):
            return hop(sbuf_l, in_l, lss, lsr, t, q, -1)

        for t in order:
            first[t].wait_recv()
            tot[t] = acc[2 * t + core] + precv[t].astype(F32)

        def push(copy, into, sbuf, t, inner):
            for q in range(CHUNKS):
                rows_of = pl.ds(q * piece, piece)

                @pl.when(inner)
                def _():
                    copy(t, q).wait_recv()
                    sbuf[t, rows_of] = (tot[t, rows_of] + into[t, rows_of].astype(F32)).astype(BF16)

                @pl.when(jnp.logical_not(inner))
                def _():
                    sbuf[t, rows_of] = tot[t, rows_of].astype(BF16)

                copy(t, q).start()

        def push_right(t):
            @pl.when(place < t)
            def _():
                push(right, in_r, sbuf_r, t, place > 0)

        def push_left(t):
            @pl.when(place > t)
            def _():
                push(left, in_l, sbuf_l, t, place < pairs - 1)

        for j in range(pairs - 1):

            @pl.when(2 * place < pairs)
            def _():
                push_right(pairs - 1 - j)
                push_left(j)

            @pl.when(2 * place >= pairs)
            def _():
                push_left(j)
                push_right(pairs - 1 - j)

        for q in range(CHUNKS):
            rows_of = pl.ds(q * piece, piece)

            @pl.when(place > 0)
            def _():
                right(place, q).wait_recv()
                tot[place, rows_of] += in_r[place, rows_of].astype(F32)

            @pl.when(place < pairs - 1)
            def _():
                left(place, q).wait_recv()
                tot[place, rows_of] += in_l[place, rows_of].astype(F32)

        sums[0][...] = tot[place]
        for t in range(pairs):
            first[t].wait_send()

            @pl.when(place < t)
            def _():
                for q in range(CHUNKS):
                    right(t, q).wait_send()

            @pl.when(place > t)
            def _():
                for q in range(CHUNKS):
                    left(t, q).wait_send()
    else:
        sums[0][...] = product(gpbuf[...], nbuf[...])
        sums[1][...] = product(abuf[...], lowbuf[...])
        sums[2][...] = product(zall[...], gall[...])

    for m in range(n_micro):

        @pl.when(sec < half)
        def _():
            values[m].wait_send()

        @pl.when(sec > 0)
        def _():
            chains[m].wait_send()

        @pl.when(sec > half)
        def _():
            skips[m].wait_send()


def finish(ig, packed, o_ig, o_skip, o_in, o_out, flat):
    o_ig[...] = ig[...]
    (fh, width) = o_in.shape
    kh = flat.shape[0]
    full = width // LANES
    tail = width % LANES
    mix = 2 * full * fh
    for i in range(full):
        cut = slice(i * LANES, (i + 1) * LANES)
        o_in[:, cut] = packed[i * fh : (i + 1) * fh, :]
        o_out[:, cut] = packed[(full + i) * fh : (full + i + 1) * fh, :]
        at = mix + fh + i * kh
        flat[:, cut] = packed[at : at + kh, :]
    rest = slice(full * LANES, width)
    at = mix + fh + full * kh
    o_in[:, rest] = packed[mix : mix + fh, 0:tail]
    o_out[:, rest] = packed[mix : mix + fh, tail : 2 * tail]
    flat[:, rest] = packed[at : at + kh, 0:tail]
    for r in range(kh):
        o_skip[:, r * width : (r + 1) * width] = flat[r : r + 1, :]


def shards(n_section, n_dp, saved_inputs, timesteps, time_table, skip_weight, ff_in, ff_out, output_cotangent):
    n_micro, rows, width = output_cotangent.shape
    hidden = ff_in.shape[1]
    pairs = n_dp // 2
    aligned = hidden % (16 * n_dp) == 0 and width % (8 * n_dp) == 0
    scatter = n_dp % 2 == 0 and aligned and width % LANES == LANES // 2
    fh = hidden // n_dp if scatter else hidden
    kh = width // n_dp if scatter else width
    every = n_micro * rows
    low = pltpu.VMEM((n_micro, width, rows), BF16)
    wide = pltpu.VMEM((width, every), BF16)
    scratch = [
        pltpu.VMEM((width, width), BF16),
        pltpu.VMEM((hidden, width), BF16),
        pltpu.VMEM((hidden, width), BF16),
        low,
        wide,
        low,
        pltpu.VMEM((n_micro, width, rows), F32),
        pltpu.VMEM((n_micro, 1, rows), F32),
        wide,
        pltpu.VMEM((hidden, every), BF16),
        pltpu.VMEM((n_micro, hidden, rows), F32),
        low,
        wide,
        pltpu.VMEM((hidden, every), BF16),
        wide,
        low,
        low,
        low,
    ] + [pltpu.SemaphoreType.DMA((n_micro,))] * 6
    turned = (
        jnp.swapaxes(saved_inputs, 2, 3),
        timesteps,
        time_table.T,
        skip_weight,
        jnp.swapaxes(ff_in, 1, 2),
        jnp.swapaxes(ff_out, 1, 2),
        jnp.swapaxes(output_cotangent, 1, 2),
    )
    scratch += [pltpu.VMEM(value.shape, value.dtype) for value in turned]
    scratch += [pltpu.SemaphoreType.DMA((7,))]
    sums = ((fh, width), (fh, width), (kh, width))
    if scatter:
        full = width // LANES
        stack = (2 * full + 1) * fh + (full + 1) * kh
        stack = -(-stack // (16 * CHUNKS)) * 16 * CHUNKS
        block = pltpu.VMEM((pairs, stack, LANES), BF16)
        scratch += [pltpu.VMEM((n_dp, stack, LANES), F32), block, block]
        scratch += [pltpu.VMEM((pairs, stack, LANES), F32), block, block, block, block]
        scratch += [pltpu.SemaphoreType.DMA((pairs,))] * 2
        scratch += [pltpu.SemaphoreType.DMA((pairs, CHUNKS))] * 4
        sums = ((stack, LANES),)
    vmem = pl.BlockSpec(memory_space=pltpu.VMEM)
    store_shape = jax.ShapeDtypeStruct(turned[0].shape, BF16)
    grad_store, *grads = pl.pallas_call(
        functools.partial(kernel, n_section, n_dp, scatter),
        out_shape=(store_shape,) + tuple(jax.ShapeDtypeStruct(shape, F32) for shape in sums),
        in_specs=[pl.BlockSpec(memory_space=pltpu.HBM)] * 7,
        out_specs=[vmem] * (1 + len(sums)),
        scratch_shapes=scratch,
        compiler_params=pltpu.CompilerParams(
            collective_id=0, has_side_effects=True, vmem_limit_bytes=60000 * 1024
        ),
    )(*turned)
    if scatter:
        grad_store, grad_skip, grad_in, grad_out = pl.pallas_call(
            finish,
            out_shape=(
                store_shape,
                jax.ShapeDtypeStruct((1, kh * width), F32),
                jax.ShapeDtypeStruct((fh, width), F32),
                jax.ShapeDtypeStruct((fh, width), F32),
            ),
            in_specs=[vmem] * 2,
            out_specs=[vmem] * 4,
            scratch_shapes=[pltpu.VMEM((kh, width), F32)],
            compiler_params=pltpu.CompilerParams(vmem_limit_bytes=60 * 1024 * 1024),
        )(grad_store, *grads)
    else:
        grad_in, grad_out, grad_skip = (
            lax.psum_scatter(value, "dp", scatter_dimension=0, tiled=True)
            for value in (grads[0], grads[1], grads[2].reshape(-1))
        )
        grad_skip = grad_skip[None]
    grad_store = jnp.swapaxes(grad_store, 2, 3)
    return (grad_store, grad_skip, grad_in[None], grad_out[None])


def solution(mesh):
    in_specs = (
        P("section", None, "dp", None),
        P(None, "dp"),
        P(),
        P("section", None, None),
        P("section", None, None),
        P("section", None, None),
        P(None, "dp", None),
    )
    out_specs = (
        P("section", None, "dp", None),
        P("section", "dp"),
        P("section", "dp", None),
        P("section", "dp", None),
    )
    body = functools.partial(shards, mesh.shape["section"], mesh.shape["dp"])
    return jax.shard_map(body, mesh=mesh, in_specs=in_specs, out_specs=out_specs, check_vma=False)
```

```python
import functools

import jax
import jax.numpy as jnp
from jax import lax
from jax.experimental import pallas as pl
from jax.experimental.pallas import tpu as pltpu
from jax.sharding import PartitionSpec as P

EPS = 1e-06
MESH = pl.DeviceIdType.MESH
F32 = jnp.float32
BF16 = jnp.bfloat16
LANES = 128
CHUNKS = 2


def contract(left, right, dims):
    return lax.dot_general(
        left, right, ((dims[0], dims[1]), ((), ())), preferred_element_type=jnp.float32
    )


def kernel(n_section, n_dp, scatter, *refs):
    outside = refs[:7]
    results = 2 if scatter else 4
    ig = refs[7]
    sums = refs[8 : 7 + results]
    refs = refs[:11] + refs[7 + results :]
    (wsk_t, win_n, wout_n, zbuf, zall, ybuf, ubuf, rbuf, nbuf, abuf, dbuf) = refs[11:22]
    (gbuf, lowbuf, gpbuf, gall, cbuf, kbuf, skbuf) = refs[22:29]
    (vs, vr, cs, cr, ks, kr) = refs[29:35]
    inside = refs[35:42]
    (x, ts, table, w_skip, w_in, w_out, cot) = inside
    loaded = refs[42]
    rs = refs[43:]
    loads = [pltpu.make_async_copy(outside[i], inside[i], loaded.at[i]) for i in range(7)]
    for i in (3, 4, 1, 2, 0, 5, 6):
        loads[i].start()
    sec = lax.axis_index("section")
    dp = lax.axis_index("dp")
    n_micro, width, rows = cot.shape
    hidden = w_in.shape[2]
    half = n_section // 2
    pairs = n_dp // 2
    core = lax.rem(dp, 2)
    place = lax.div(dp, 2)
    mate = dp + 1 - 2 * core

    def remote(src, dst, send, recv, **where):
        return pltpu.make_async_remote_copy(
            src_ref=src, dst_ref=dst, send_sem=send, recv_sem=recv, device_id=where, device_id_type=MESH
        )

    barrier = pltpu.get_barrier_semaphore()
    count = 0
    for k in range(1, n_section):
        pl.semaphore_signal(
            barrier, inc=1, device_id={"section": lax.rem(sec + k, n_section)}, device_id_type=MESH
        )
        count += 1
    if scatter:
        pl.semaphore_signal(barrier, inc=1, device_id={"dp": mate}, device_id_type=MESH)
        count += 1
        for k in range(1, pairs):
            other = lax.rem(place + k, pairs) * 2 + core
            pl.semaphore_signal(barrier, inc=1, device_id={"dp": other}, device_id_type=MESH)
            count += 1

    mirror = n_section - 1 - sec
    below = lax.max(sec - 1, 0)
    values = [remote(ybuf.at[m], zbuf.at[m], vs.at[m], vr.at[m], section=mirror) for m in range(n_micro)]
    chains = [remote(cbuf.at[m], gbuf.at[m], cs.at[m], cr.at[m], section=below) for m in range(n_micro)]
    skips = [remote(kbuf.at[m], skbuf.at[m], ks.at[m], kr.at[m], section=mirror) for m in range(n_micro)]

    def forward(m):
        span = slice(m * rows, (m + 1) * rows)
        side = zbuf[m]
        zall[:, span] = side
        united = x[0, m].astype(F32) + jnp.dot(wsk_t[...], side, preferred_element_type=F32)
        recip = lax.rsqrt(jnp.mean(united * united, axis=0, keepdims=True) + EPS)
        normed = (united * recip).astype(BF16)
        preact = jnp.dot(win_n[...], normed, preferred_element_type=F32)
        sigma = jax.nn.sigmoid(preact)
        active = (preact * sigma).astype(BF16)
        ubuf[m] = united
        rbuf[m] = recip
        nbuf[:, span] = normed
        abuf[:, span] = active
        dbuf[m] = sigma * (1.0 + preact * (1.0 - sigma))
        return united, active

    loads[3].wait()
    wsk_t[...] = w_skip[0].T
    loads[4].wait()
    win_n[...] = w_in[0].T
    for i in (1, 2, 0, 5):
        loads[i].wait()

    @pl.when(sec < half)
    def _():
        levels = lax.broadcasted_iota(jnp.int32, (table.shape[1], rows), 0)
        for m in range(n_micro):
            onehot = (levels == ts[m : m + 1, :]).astype(F32).astype(BF16)
            zbuf[m] = jnp.dot(table[...], onehot, preferred_element_type=F32).astype(BF16)
            united, active = forward(m)
            output = united + jnp.dot(w_out[0], active, preferred_element_type=F32)
            ybuf[m] = output.astype(BF16)
            if m == 0:
                pl.semaphore_wait(barrier, count)
            values[m].start()

    wout_n[...] = w_out[0].T
    loads[6].wait()

    @pl.when(sec >= half - 1)
    def _():
        skbuf[...] = jnp.zeros_like(skbuf)

    @pl.when(sec >= half)
    def _():
        pl.semaphore_wait(barrier, count)

    for m in range(n_micro):

        @pl.when(sec >= half)
        def _():
            values[m].wait_recv()
            forward(m)

        @pl.when(sec == n_section - 1)
        def _():
            gbuf[m] = cot[m]

        @pl.when(sec < n_section - 1)
        def _():
            chains[m].wait_recv()

        @pl.when(sec < half - 1)
        def _():
            skips[m].wait_recv()

        span = slice(m * rows, (m + 1) * rows)
        grad_out = gbuf[m].astype(F32) + skbuf[m].astype(F32)
        grad_low = grad_out.astype(BF16)
        lowbuf[:, span] = grad_low
        grad_act = jnp.dot(wout_n[...], grad_low, preferred_element_type=F32)
        grad_pre = (grad_act * dbuf[m]).astype(BF16)
        gpbuf[:, span] = grad_pre
        grad_norm = jnp.dot(w_in[0], grad_pre, preferred_element_type=F32)
        united = ubuf[m]
        recip = rbuf[m]
        grad_united = (
            grad_out
            + recip * grad_norm
            - united * recip**3 * jnp.mean(grad_norm * united, axis=0, keepdims=True)
        )
        low = grad_united.astype(BF16)

        @pl.when(sec != half)
        def _():
            cbuf[m] = low

            @pl.when(sec > 0)
            def _():
                chains[m].start()

        @pl.when(sec >= half)
        def _():
            back = jnp.dot(w_skip[0], low, preferred_element_type=F32).astype(BF16)

            @pl.when(sec == half)
            def _():
                cbuf[m] = (low.astype(F32) + back.astype(F32)).astype(BF16)
                chains[m].start()

            @pl.when(sec > half)
            def _():
                kbuf[m] = back
                skips[m].start()

        ig[0, m] = low
        gall[:, span] = low

    def product(left, right):
        return contract(left, right, ((1,), (1,)))

    if scatter:
        (acc, pbuf, precv, tot, sbuf_r, sbuf_l, in_r, in_l, ps, pr, rss, rsr, lss, lsr) = rs
        fh = hidden // n_dp
        kh = width // n_dp
        full = width // LANES
        tail = width % LANES
        stack = acc.shape[1]
        piece = stack // CHUNKS
        mix = 2 * full * fh
        order = []
        for t in range(pairs):
            k = pairs - 1 - t // 2 if t % 2 == 0 else t // 2
            order.append(k)
        first = [
            remote(pbuf.at[t], precv.at[t], ps.at[t], pr.at[t], dp=mate) for t in range(pairs)
        ]
        def hop(sbuf, into, send, recv, t, q, step):
            rows_of = pl.ds(q * piece, piece)
            at = jnp.clip(place + step, 0, pairs - 1) * 2 + core
            return remote(
                sbuf.at[t, rows_of], into.at[t, rows_of], send.at[t, q], recv.at[t, q], dp=at
            )

        def right(t, q):
            return hop(sbuf_r, in_r, rss, rsr, t, q, 1)

        def left(t, q):
            return hop(sbuf_l, in_l, lss, lsr, t, q, -1)

        def meet(t):
            first[t].wait_recv()
            tot[t] = acc[2 * t + core] + precv[t].astype(F32)

        def open_line(copy, sbuf, t):
            for q in range(CHUNKS):
                rows_of = pl.ds(q * piece, piece)
                sbuf[t, rows_of] = tot[t, rows_of].astype(BF16)
                copy(t, q).start()

        for i_t, t in enumerate(order):
            fspan = slice(2 * t * fh, 2 * (t + 1) * fh)
            kspan = slice(2 * t * kh, 2 * (t + 1) * kh)
            d_out = product(abuf[fspan, :], lowbuf[...])
            d_in = product(gpbuf[fspan, :], nbuf[...])
            d_skip = product(zall[kspan, :], gall[...])
            for c in range(2):
                d = 2 * t + c
                for i in range(full):
                    cut = slice(i * LANES, (i + 1) * LANES)
                    acc[d, i * fh : (i + 1) * fh, :] = d_in[c * fh : (c + 1) * fh, cut]
                    acc[d, (full + i) * fh : (full + i + 1) * fh, :] = d_out[c * fh : (c + 1) * fh, cut]
                    at = mix + fh + i * kh
                    acc[d, at : at + kh, :] = d_skip[c * kh : (c + 1) * kh, cut]
                rest = slice(full * LANES, width)
                acc[d, mix : mix + fh, 0:tail] = d_in[c * fh : (c + 1) * fh, rest]
                acc[d, mix : mix + fh, tail : 2 * tail] = d_out[c * fh : (c + 1) * fh, rest]
                at = mix + fh + full * kh
                acc[d, at:stack, :] = jnp.zeros((stack - at, LANES), F32)
                acc[d, at : at + kh, 0:tail] = d_skip[c * kh : (c + 1) * kh, rest]
            pbuf[t] = acc[2 * t + 1 - core].astype(BF16)
            first[t].start()
            if i_t == 1:
                meet(order[0])
                meet(order[1])

                @pl.when(place == 0)
                def _():
                    open_line(right, sbuf_r, pairs - 1)

                @pl.when(place == pairs - 1)
                def _():
                    open_line(left, sbuf_l, 0)

        for t in order[2:]:
            meet(t)

        def push(copy, into, sbuf, t, inner):
            for q in range(CHUNKS):
                rows_of = pl.ds(q * piece, piece)

                @pl.when(inner)
                def _():
                    copy(t, q).wait_recv()
                    sbuf[t, rows_of] = (tot[t, rows_of] + into[t, rows_of].astype(F32)).astype(BF16)

                @pl.when(jnp.logical_not(inner))
                def _():
                    sbuf[t, rows_of] = tot[t, rows_of].astype(BF16)

                copy(t, q).start()

        def push_right(t):
            @pl.when((place < t) & (place > 0) if t == pairs - 1 else place < t)
            def _():
                push(right, in_r, sbuf_r, t, place > 0)

        def push_left(t):
            @pl.when((place > t) & (place < pairs - 1) if t == 0 else place > t)
            def _():
                push(left, in_l, sbuf_l, t, place < pairs - 1)

        for j in range(pairs - 1):

            @pl.when(2 * place < pairs)
            def _():
                push_right(pairs - 1 - j)
                push_left(j)

            @pl.when(2 * place >= pairs)
            def _():
                push_left(j)
                push_right(pairs - 1 - j)

        for q in range(CHUNKS):
            rows_of = pl.ds(q * piece, piece)

            @pl.when(place > 0)
            def _():
                right(place, q).wait_recv()
                tot[place, rows_of] += in_r[place, rows_of].astype(F32)

            @pl.when(place < pairs - 1)
            def _():
                left(place, q).wait_recv()
                tot[place, rows_of] += in_l[place, rows_of].astype(F32)

        sums[0][...] = tot[place]
        for t in range(pairs):
            first[t].wait_send()

            @pl.when(place < t)
            def _():
                for q in range(CHUNKS):
                    right(t, q).wait_send()

            @pl.when(place > t)
            def _():
                for q in range(CHUNKS):
                    left(t, q).wait_send()
    else:
        sums[0][...] = product(gpbuf[...], nbuf[...])
        sums[1][...] = product(abuf[...], lowbuf[...])
        sums[2][...] = product(zall[...], gall[...])

    for m in range(n_micro):

        @pl.when(sec < half)
        def _():
            values[m].wait_send()

        @pl.when(sec > 0)
        def _():
            chains[m].wait_send()

        @pl.when(sec > half)
        def _():
            skips[m].wait_send()


def finish(ig, packed, o_ig, o_skip, o_in, o_out, flat):
    o_ig[...] = ig[...]
    (fh, width) = o_in.shape
    kh = flat.shape[0]
    full = width // LANES
    tail = width % LANES
    mix = 2 * full * fh
    for i in range(full):
        cut = slice(i * LANES, (i + 1) * LANES)
        o_in[:, cut] = packed[i * fh : (i + 1) * fh, :]
        o_out[:, cut] = packed[(full + i) * fh : (full + i + 1) * fh, :]
        at = mix + fh + i * kh
        flat[:, cut] = packed[at : at + kh, :]
    rest = slice(full * LANES, width)
    at = mix + fh + full * kh
    o_in[:, rest] = packed[mix : mix + fh, 0:tail]
    o_out[:, rest] = packed[mix : mix + fh, tail : 2 * tail]
    flat[:, rest] = packed[at : at + kh, 0:tail]
    for r in range(kh):
        o_skip[:, r * width : (r + 1) * width] = flat[r : r + 1, :]


def shards(n_section, n_dp, saved_inputs, timesteps, time_table, skip_weight, ff_in, ff_out, output_cotangent):
    n_micro, rows, width = output_cotangent.shape
    hidden = ff_in.shape[1]
    pairs = n_dp // 2
    aligned = hidden % (16 * n_dp) == 0 and width % (8 * n_dp) == 0
    scatter = n_dp % 2 == 0 and pairs > 1 and aligned and width % LANES == LANES // 2
    fh = hidden // n_dp if scatter else hidden
    kh = width // n_dp if scatter else width
    every = n_micro * rows
    low = pltpu.VMEM((n_micro, width, rows), BF16)
    wide = pltpu.VMEM((width, every), BF16)
    scratch = [
        pltpu.VMEM((width, width), BF16),
        pltpu.VMEM((hidden, width), BF16),
        pltpu.VMEM((hidden, width), BF16),
        low,
        wide,
        low,
        pltpu.VMEM((n_micro, width, rows), F32),
        pltpu.VMEM((n_micro, 1, rows), F32),
        wide,
        pltpu.VMEM((hidden, every), BF16),
        pltpu.VMEM((n_micro, hidden, rows), F32),
        low,
        wide,
        pltpu.VMEM((hidden, every), BF16),
        wide,
        low,
        low,
        low,
    ] + [pltpu.SemaphoreType.DMA((n_micro,))] * 6
    turned = (
        jnp.swapaxes(saved_inputs, 2, 3),
        timesteps,
        time_table.T,
        skip_weight,
        jnp.swapaxes(ff_in, 1, 2),
        jnp.swapaxes(ff_out, 1, 2),
        jnp.swapaxes(output_cotangent, 1, 2),
    )
    scratch += [pltpu.VMEM(value.shape, value.dtype) for value in turned]
    scratch += [pltpu.SemaphoreType.DMA((7,))]
    sums = ((fh, width), (fh, width), (kh, width))
    if scatter:
        full = width // LANES
        stack = (2 * full + 1) * fh + (full + 1) * kh
        stack = -(-stack // (16 * CHUNKS)) * 16 * CHUNKS
        block = pltpu.VMEM((pairs, stack, LANES), BF16)
        scratch += [pltpu.VMEM((n_dp, stack, LANES), F32), block, block]
        scratch += [pltpu.VMEM((pairs, stack, LANES), F32), block, block, block, block]
        scratch += [pltpu.SemaphoreType.DMA((pairs,))] * 2
        scratch += [pltpu.SemaphoreType.DMA((pairs, CHUNKS))] * 4
        sums = ((stack, LANES),)
    vmem = pl.BlockSpec(memory_space=pltpu.VMEM)
    store_shape = jax.ShapeDtypeStruct(turned[0].shape, BF16)
    grad_store, *grads = pl.pallas_call(
        functools.partial(kernel, n_section, n_dp, scatter),
        out_shape=(store_shape,) + tuple(jax.ShapeDtypeStruct(shape, F32) for shape in sums),
        in_specs=[pl.BlockSpec(memory_space=pltpu.HBM)] * 7,
        out_specs=[vmem] * (1 + len(sums)),
        scratch_shapes=scratch,
        compiler_params=pltpu.CompilerParams(
            collective_id=0, has_side_effects=True, vmem_limit_bytes=60000 * 1024
        ),
    )(*turned)
    if scatter:
        grad_store, grad_skip, grad_in, grad_out = pl.pallas_call(
            finish,
            out_shape=(
                store_shape,
                jax.ShapeDtypeStruct((1, kh * width), F32),
                jax.ShapeDtypeStruct((fh, width), F32),
                jax.ShapeDtypeStruct((fh, width), F32),
            ),
            in_specs=[vmem] * 2,
            out_specs=[vmem] * 4,
            scratch_shapes=[pltpu.VMEM((kh, width), F32)],
            compiler_params=pltpu.CompilerParams(vmem_limit_bytes=60 * 1024 * 1024),
        )(grad_store, *grads)
    else:
        grad_in, grad_out, grad_skip = (
            lax.psum_scatter(value, "dp", scatter_dimension=0, tiled=True)
            for value in (grads[0], grads[1], grads[2].reshape(-1))
        )
        grad_skip = grad_skip[None]
    grad_store = jnp.swapaxes(grad_store, 2, 3)
    return (grad_store, grad_skip, grad_in[None], grad_out[None])


def solution(mesh):
    in_specs = (
        P("section", None, "dp", None),
        P(None, "dp"),
        P(),
        P("section", None, None),
        P("section", None, None),
        P("section", None, None),
        P(None, "dp", None),
    )
    out_specs = (
        P("section", None, "dp", None),
        P("section", "dp"),
        P("section", "dp", None),
        P("section", "dp", None),
    )
    body = functools.partial(shards, mesh.shape["section"], mesh.shape["dp"])
    return jax.shard_map(body, mesh=mesh, in_specs=in_specs, out_specs=out_specs, check_vma=False)
```

```python
import functools

import jax
import jax.numpy as jnp
from jax import lax
from jax.experimental import pallas as pl
from jax.experimental.pallas import tpu as pltpu
from jax.sharding import PartitionSpec as P

EPS = 1e-06
MESH = pl.DeviceIdType.MESH
F32 = jnp.float32
BF16 = jnp.bfloat16
LANES = 128
CHUNKS = 1


def contract(left, right, dims):
    return lax.dot_general(
        left, right, ((dims[0], dims[1]), ((), ())), preferred_element_type=jnp.float32
    )


def kernel(n_section, n_dp, scatter, *refs):
    outside = refs[:7]
    results = 2 if scatter else 4
    ig = refs[7]
    sums = refs[8 : 7 + results]
    refs = refs[:11] + refs[7 + results :]
    (wsk_t, win_n, wout_n, zbuf, zall, ybuf, ubuf, rbuf, nbuf, abuf, dbuf) = refs[11:22]
    (gbuf, lowbuf, gpbuf, gall, cbuf, kbuf, skbuf) = refs[22:29]
    (vs, vr, cs, cr, ks, kr) = refs[29:35]
    inside = refs[35:42]
    (x, ts, table, w_skip, w_in, w_out, cot) = inside
    loaded = refs[42]
    rs = refs[43:]
    loads = [pltpu.make_async_copy(outside[i], inside[i], loaded.at[i]) for i in range(7)]
    for i in (3, 4, 1, 2, 0, 5, 6):
        loads[i].start()
    sec = lax.axis_index("section")
    dp = lax.axis_index("dp")
    n_micro, width, rows = cot.shape
    hidden = w_in.shape[2]
    half = n_section // 2
    pairs = n_dp // 2
    core = lax.rem(dp, 2)
    place = lax.div(dp, 2)
    mate = dp + 1 - 2 * core

    def remote(src, dst, send, recv, **where):
        return pltpu.make_async_remote_copy(
            src_ref=src, dst_ref=dst, send_sem=send, recv_sem=recv, device_id=where, device_id_type=MESH
        )

    barrier = pltpu.get_barrier_semaphore()
    count = 0
    for k in range(1, n_section):
        pl.semaphore_signal(
            barrier, inc=1, device_id={"section": lax.rem(sec + k, n_section)}, device_id_type=MESH
        )
        count += 1
    if scatter:
        pl.semaphore_signal(barrier, inc=1, device_id={"dp": mate}, device_id_type=MESH)
        count += 1
        for k in range(1, pairs):
            other = lax.rem(place + k, pairs) * 2 + core
            pl.semaphore_signal(barrier, inc=1, device_id={"dp": other}, device_id_type=MESH)
            count += 1

    mirror = n_section - 1 - sec
    below = lax.max(sec - 1, 0)
    values = [remote(ybuf.at[m], zbuf.at[m], vs.at[m], vr.at[m], section=mirror) for m in range(n_micro)]
    chains = [remote(cbuf.at[m], gbuf.at[m], cs.at[m], cr.at[m], section=below) for m in range(n_micro)]
    skips = [remote(kbuf.at[m], skbuf.at[m], ks.at[m], kr.at[m], section=mirror) for m in range(n_micro)]

    def forward(m):
        span = slice(m * rows, (m + 1) * rows)
        side = zbuf[m]
        zall[:, span] = side
        united = x[0, m].astype(F32) + jnp.dot(wsk_t[...], side, preferred_element_type=F32)
        recip = lax.rsqrt(jnp.mean(united * united, axis=0, keepdims=True) + EPS)
        normed = (united * recip).astype(BF16)
        preact = jnp.dot(win_n[...], normed, preferred_element_type=F32)
        sigma = jax.nn.sigmoid(preact)
        active = (preact * sigma).astype(BF16)
        ubuf[m] = united
        rbuf[m] = recip
        nbuf[:, span] = normed
        abuf[:, span] = active
        dbuf[m] = sigma * (1.0 + preact * (1.0 - sigma))
        return united, active

    loads[3].wait()
    wsk_t[...] = w_skip[0].T
    loads[4].wait()
    win_n[...] = w_in[0].T
    for i in (1, 2, 0, 5):
        loads[i].wait()

    @pl.when(sec < half)
    def _():
        levels = lax.broadcasted_iota(jnp.int32, (table.shape[1], rows), 0)
        for m in range(n_micro):
            onehot = (levels == ts[m : m + 1, :]).astype(F32).astype(BF16)
            zbuf[m] = jnp.dot(table[...], onehot, preferred_element_type=F32).astype(BF16)
            united, active = forward(m)
            output = united + jnp.dot(w_out[0], active, preferred_element_type=F32)
            ybuf[m] = output.astype(BF16)
            if m == 0:
                pl.semaphore_wait(barrier, count)
            values[m].start()

    wout_n[...] = w_out[0].T
    loads[6].wait()

    @pl.when(sec >= half - 1)
    def _():
        skbuf[...] = jnp.zeros_like(skbuf)

    @pl.when(sec >= half)
    def _():
        pl.semaphore_wait(barrier, count)

    for m in range(n_micro):

        @pl.when(sec >= half)
        def _():
            values[m].wait_recv()
            forward(m)

        @pl.when(sec == n_section - 1)
        def _():
            gbuf[m] = cot[m]

        @pl.when(sec < n_section - 1)
        def _():
            chains[m].wait_recv()

        @pl.when(sec < half - 1)
        def _():
            skips[m].wait_recv()

        span = slice(m * rows, (m + 1) * rows)
        grad_out = gbuf[m].astype(F32) + skbuf[m].astype(F32)
        grad_low = grad_out.astype(BF16)
        lowbuf[:, span] = grad_low
        grad_act = jnp.dot(wout_n[...], grad_low, preferred_element_type=F32)
        grad_pre = (grad_act * dbuf[m]).astype(BF16)
        gpbuf[:, span] = grad_pre
        grad_norm = jnp.dot(w_in[0], grad_pre, preferred_element_type=F32)
        united = ubuf[m]
        recip = rbuf[m]
        grad_united = (
            grad_out
            + recip * grad_norm
            - united * recip**3 * jnp.mean(grad_norm * united, axis=0, keepdims=True)
        )
        low = grad_united.astype(BF16)

        @pl.when(sec != half)
        def _():
            cbuf[m] = low

            @pl.when(sec > 0)
            def _():
                chains[m].start()

        @pl.when(sec >= half)
        def _():
            back = jnp.dot(w_skip[0], low, preferred_element_type=F32).astype(BF16)

            @pl.when(sec == half)
            def _():
                cbuf[m] = (low.astype(F32) + back.astype(F32)).astype(BF16)
                chains[m].start()

            @pl.when(sec > half)
            def _():
                kbuf[m] = back
                skips[m].start()

        ig[0, m] = low
        gall[:, span] = low

    def product(left, right):
        return contract(left, right, ((1,), (1,)))

    if scatter:
        (acc, pbuf, precv, tot, sbuf_r, sbuf_l, in_r, in_l, ps, pr, rss, rsr, lss, lsr) = rs
        fh = hidden // n_dp
        kh = width // n_dp
        full = width // LANES
        tail = width % LANES
        stack = acc.shape[1]
        piece = stack // CHUNKS
        mix = 2 * full * fh
        order = []
        for t in range(pairs):
            k = pairs - 1 - t // 2 if t % 2 == 0 else t // 2
            order.append(k)
        first = [
            remote(pbuf.at[t], precv.at[t], ps.at[t], pr.at[t], dp=mate) for t in range(pairs)
        ]
        def hop(sbuf, into, send, recv, t, q, step):
            rows_of = pl.ds(q * piece, piece)
            at = jnp.clip(place + step, 0, pairs - 1) * 2 + core
            return remote(
                sbuf.at[t, rows_of], into.at[t, rows_of], send.at[t, q], recv.at[t, q], dp=at
            )

        def right(t, q):
            return hop(sbuf_r, in_r, rss, rsr, t, q, 1)

        def left(t, q):
            return hop(sbuf_l, in_l, lss, lsr, t, q, -1)

        def meet(t):
            first[t].wait_recv()
            tot[t] = acc[2 * t + core] + precv[t].astype(F32)

        def open_line(copy, sbuf, t):
            for q in range(CHUNKS):
                rows_of = pl.ds(q * piece, piece)
                sbuf[t, rows_of] = tot[t, rows_of].astype(BF16)
                copy(t, q).start()

        for i_t, t in enumerate(order):
            fspan = slice(2 * t * fh, 2 * (t + 1) * fh)
            kspan = slice(2 * t * kh, 2 * (t + 1) * kh)
            d_out = product(abuf[fspan, :], lowbuf[...])
            d_in = product(gpbuf[fspan, :], nbuf[...])
            d_skip = product(zall[kspan, :], gall[...])
            for c in range(2):
                d = 2 * t + c
                for i in range(full):
                    cut = slice(i * LANES, (i + 1) * LANES)
                    acc[d, i * fh : (i + 1) * fh, :] = d_in[c * fh : (c + 1) * fh, cut]
                    acc[d, (full + i) * fh : (full + i + 1) * fh, :] = d_out[c * fh : (c + 1) * fh, cut]
                    at = mix + fh + i * kh
                    acc[d, at : at + kh, :] = d_skip[c * kh : (c + 1) * kh, cut]
                rest = slice(full * LANES, width)
                acc[d, mix : mix + fh, 0:tail] = d_in[c * fh : (c + 1) * fh, rest]
                acc[d, mix : mix + fh, tail : 2 * tail] = d_out[c * fh : (c + 1) * fh, rest]
                at = mix + fh + full * kh
                acc[d, at:stack, :] = jnp.zeros((stack - at, LANES), F32)
                acc[d, at : at + kh, 0:tail] = d_skip[c * kh : (c + 1) * kh, rest]
            pbuf[t] = acc[2 * t + 1 - core].astype(BF16)
            first[t].start()
            if i_t == 1:
                meet(order[0])
                meet(order[1])

                @pl.when(place == 0)
                def _():
                    open_line(right, sbuf_r, pairs - 1)

                @pl.when(place == pairs - 1)
                def _():
                    open_line(left, sbuf_l, 0)

        for t in order[2:]:
            meet(t)

        def push(copy, into, sbuf, t, inner):
            for q in range(CHUNKS):
                rows_of = pl.ds(q * piece, piece)

                @pl.when(inner)
                def _():
                    copy(t, q).wait_recv()
                    sbuf[t, rows_of] = (tot[t, rows_of] + into[t, rows_of].astype(F32)).astype(BF16)

                @pl.when(jnp.logical_not(inner))
                def _():
                    sbuf[t, rows_of] = tot[t, rows_of].astype(BF16)

                copy(t, q).start()

        def push_right(t):
            @pl.when((place < t) & (place > 0) if t == pairs - 1 else place < t)
            def _():
                push(right, in_r, sbuf_r, t, place > 0)

        def push_left(t):
            @pl.when((place > t) & (place < pairs - 1) if t == 0 else place > t)
            def _():
                push(left, in_l, sbuf_l, t, place < pairs - 1)

        for j in range(pairs - 1):

            @pl.when(2 * place < pairs)
            def _():
                push_right(pairs - 1 - j)
                push_left(j)

            @pl.when(2 * place >= pairs)
            def _():
                push_left(j)
                push_right(pairs - 1 - j)

        for q in range(CHUNKS):
            rows_of = pl.ds(q * piece, piece)

            @pl.when(place > 0)
            def _():
                right(place, q).wait_recv()
                tot[place, rows_of] += in_r[place, rows_of].astype(F32)

            @pl.when(place < pairs - 1)
            def _():
                left(place, q).wait_recv()
                tot[place, rows_of] += in_l[place, rows_of].astype(F32)

        sums[0][...] = tot[place]
        for t in range(pairs):
            first[t].wait_send()

            @pl.when(place < t)
            def _():
                for q in range(CHUNKS):
                    right(t, q).wait_send()

            @pl.when(place > t)
            def _():
                for q in range(CHUNKS):
                    left(t, q).wait_send()
    else:
        sums[0][...] = product(gpbuf[...], nbuf[...])
        sums[1][...] = product(abuf[...], lowbuf[...])
        sums[2][...] = product(zall[...], gall[...])

    for m in range(n_micro):

        @pl.when(sec < half)
        def _():
            values[m].wait_send()

        @pl.when(sec > 0)
        def _():
            chains[m].wait_send()

        @pl.when(sec > half)
        def _():
            skips[m].wait_send()


def finish(ig, packed, o_ig, o_skip, o_in, o_out, flat):
    o_ig[...] = ig[...]
    (fh, width) = o_in.shape
    kh = flat.shape[0]
    full = width // LANES
    tail = width % LANES
    mix = 2 * full * fh
    for i in range(full):
        cut = slice(i * LANES, (i + 1) * LANES)
        o_in[:, cut] = packed[i * fh : (i + 1) * fh, :]
        o_out[:, cut] = packed[(full + i) * fh : (full + i + 1) * fh, :]
        at = mix + fh + i * kh
        flat[:, cut] = packed[at : at + kh, :]
    rest = slice(full * LANES, width)
    at = mix + fh + full * kh
    o_in[:, rest] = packed[mix : mix + fh, 0:tail]
    o_out[:, rest] = packed[mix : mix + fh, tail : 2 * tail]
    flat[:, rest] = packed[at : at + kh, 0:tail]
    for r in range(kh):
        o_skip[:, r * width : (r + 1) * width] = flat[r : r + 1, :]


def shards(n_section, n_dp, saved_inputs, timesteps, time_table, skip_weight, ff_in, ff_out, output_cotangent):
    n_micro, rows, width = output_cotangent.shape
    hidden = ff_in.shape[1]
    pairs = n_dp // 2
    aligned = hidden % (16 * n_dp) == 0 and width % (8 * n_dp) == 0
    scatter = n_dp % 2 == 0 and pairs > 1 and aligned and width % LANES == LANES // 2
    fh = hidden // n_dp if scatter else hidden
    kh = width // n_dp if scatter else width
    every = n_micro * rows
    low = pltpu.VMEM((n_micro, width, rows), BF16)
    wide = pltpu.VMEM((width, every), BF16)
    scratch = [
        pltpu.VMEM((width, width), BF16),
        pltpu.VMEM((hidden, width), BF16),
        pltpu.VMEM((hidden, width), BF16),
        low,
        wide,
        low,
        pltpu.VMEM((n_micro, width, rows), F32),
        pltpu.VMEM((n_micro, 1, rows), F32),
        wide,
        pltpu.VMEM((hidden, every), BF16),
        pltpu.VMEM((n_micro, hidden, rows), F32),
        low,
        wide,
        pltpu.VMEM((hidden, every), BF16),
        wide,
        low,
        low,
        low,
    ] + [pltpu.SemaphoreType.DMA((n_micro,))] * 6
    turned = (
        jnp.swapaxes(saved_inputs, 2, 3),
        timesteps,
        time_table.T,
        skip_weight,
        jnp.swapaxes(ff_in, 1, 2),
        jnp.swapaxes(ff_out, 1, 2),
        jnp.swapaxes(output_cotangent, 1, 2),
    )
    scratch += [pltpu.VMEM(value.shape, value.dtype) for value in turned]
    scratch += [pltpu.SemaphoreType.DMA((7,))]
    sums = ((fh, width), (fh, width), (kh, width))
    if scatter:
        full = width // LANES
        stack = (2 * full + 1) * fh + (full + 1) * kh
        stack = -(-stack // (16 * CHUNKS)) * 16 * CHUNKS
        block = pltpu.VMEM((pairs, stack, LANES), BF16)
        scratch += [pltpu.VMEM((n_dp, stack, LANES), F32), block, block]
        scratch += [pltpu.VMEM((pairs, stack, LANES), F32), block, block, block, block]
        scratch += [pltpu.SemaphoreType.DMA((pairs,))] * 2
        scratch += [pltpu.SemaphoreType.DMA((pairs, CHUNKS))] * 4
        sums = ((stack, LANES),)
    vmem = pl.BlockSpec(memory_space=pltpu.VMEM)
    store_shape = jax.ShapeDtypeStruct(turned[0].shape, BF16)
    grad_store, *grads = pl.pallas_call(
        functools.partial(kernel, n_section, n_dp, scatter),
        out_shape=(store_shape,) + tuple(jax.ShapeDtypeStruct(shape, F32) for shape in sums),
        in_specs=[pl.BlockSpec(memory_space=pltpu.HBM)] * 7,
        out_specs=[vmem] * (1 + len(sums)),
        scratch_shapes=scratch,
        compiler_params=pltpu.CompilerParams(
            collective_id=0, has_side_effects=True, vmem_limit_bytes=60000 * 1024
        ),
    )(*turned)
    if scatter:
        grad_store, grad_skip, grad_in, grad_out = pl.pallas_call(
            finish,
            out_shape=(
                store_shape,
                jax.ShapeDtypeStruct((1, kh * width), F32),
                jax.ShapeDtypeStruct((fh, width), F32),
                jax.ShapeDtypeStruct((fh, width), F32),
            ),
            in_specs=[vmem] * 2,
            out_specs=[vmem] * 4,
            scratch_shapes=[pltpu.VMEM((kh, width), F32)],
            compiler_params=pltpu.CompilerParams(vmem_limit_bytes=60 * 1024 * 1024),
        )(grad_store, *grads)
    else:
        grad_in, grad_out, grad_skip = (
            lax.psum_scatter(value, "dp", scatter_dimension=0, tiled=True)
            for value in (grads[0], grads[1], grads[2].reshape(-1))
        )
        grad_skip = grad_skip[None]
    grad_store = jnp.swapaxes(grad_store, 2, 3)
    return (grad_store, grad_skip, grad_in[None], grad_out[None])


def solution(mesh):
    in_specs = (
        P("section", None, "dp", None),
        P(None, "dp"),
        P(),
        P("section", None, None),
        P("section", None, None),
        P("section", None, None),
        P(None, "dp", None),
    )
    out_specs = (
        P("section", None, "dp", None),
        P("section", "dp"),
        P("section", "dp", None),
        P("section", "dp", None),
    )
    body = functools.partial(shards, mesh.shape["section"], mesh.shape["dp"])
    return jax.shard_map(body, mesh=mesh, in_specs=in_specs, out_specs=out_specs, check_vma=False)
```
